128 devices in a mesh: seq: 16 (over x, z_hi, core), tp: 8 (over z_lo, y).
Axes of the slice: x: 4, y: 4, z: 4 (z_hi: 2, z_lo: 2; z = z_hi * 2 + z_lo), core: 2. Of those that a mesh axis runs over, the one named last changes fastest.
Arguments:
- states: bfloat16 [4096, 4096], P('seq', 'tp'), may hold values from -1.5 to 1.5
- doc_lengths: int32 [4], replicated, may hold values from 1 to 2048, 4096 in all
- attn_gain: float32 [4096], replicated, may hold values from 0.9 to 6
- query_weight: bfloat16 [4096, 4096], P(None, 'tp'), may hold values from -0.09375 to 0.09375
- key_weight: bfloat16 [4096, 1024], P(None, 'tp'), may hold values from -0.09375 to 0.09375
- value_weight: bfloat16 [4096, 1024], P(None, 'tp'), may hold values from -0.09375 to 0.09375
- output_weight: bfloat16 [4096, 4096], P('tp'), may hold values from -0.5 to 0.5
- mlp_gain: float32 [4096], replicated, may hold values from 0.5 to 1.5
- gate_weight: bfloat16 [4096, 7168], P('seq', 'tp'), may hold values from -0.09375 to 0.09375
- up_weight: bfloat16 [4096, 7168], P('seq', 'tp'), may hold values from -0.09375 to 0.09375
- down_weight: bfloat16 [7168, 4096], P('tp', 'seq'), may hold values from -0.0625 to 0.0625
Outputs:
- layer_out: bfloat16 [4096, 4096], P('seq', 'tp')
The draws below stay inside these ranges and needn't reach their ends.
Inputs may be any that keep to these rules, and one draw needn't show every extreme that they name: `doc_lengths`: 4 documents that fill the 4096 tokens in order.
All inputs are finite; a program needn't handle non-finite values.
Results may differ from the reference program's by a relative error of at most 0.014.
The reference program's roundings to bfloat16 on the way count: a program that leaves them out, or rounds other values in their place, can miss the bound.
Values may be sent and summed in bfloat16 or wider, within the bound.
A program may use at most 128 MiB of HBM per device.

```python
import math
import jax
import jax.numpy as jnp
import numpy as np
from jax import lax

D = 4096
HEADS = 32
KV_HEADS = 8
HD = 128
FF = 7168
SEQS = 4
TOKENS = 4096


def draw_attn_gain(key, part):
    return jax.random.uniform(key, (D,), jnp.float32, 0.9, 1.1)


def block_scale(key, extent, split, smallest, high):
    loudness = 1.0
    for axis_at, blocks in split:
        heights = jax.random.uniform(jax.random.fold_in(jax.random.fold_in(key, 6), axis_at), (blocks,), jnp.float32, smallest / len(split), high / len(split))
        loudness = loudness * jnp.repeat(jnp.exp(heights), extent[axis_at] // blocks).reshape((-1,) + (1,) * (len(extent) - 1 - axis_at))
    return loudness


def profile(amount, total, most, skew):
    portions = [(1 << 20) // math.isqrt(standing ** skew) + 1 for standing in range(2, amount + 1)]
    rest, holding = total - most - (amount - 1), [1] * (amount - 1)
    while rest > 0:
        candidates = [i for i in range(amount - 1) if holding[i] < most]
        mass, remaining = sum([portions[i] for i in candidates]), rest
        for i in candidates:
            extra = min(most - holding[i], max(1, remaining * portions[i] // mass), rest)
            holding[i] = holding[i] + extra
            rest = rest - extra
    return np.array([most] + holding)


def ragged(own_key, count, total, bound, skew):
    if count == 2:
        one = jax.random.randint(own_key, (), max(1, total - bound), min(bound, total - 1) + 1)
        return jnp.stack([one, total - one])
    tallies = jnp.asarray(profile(count, total, bound, skew), jnp.int32)
    twos = (count - 1) // 2
    source_of, receiver = tallies[1:1 + 2 * twos:2], tallies[2:2 + 2 * twos:2]
    room = jnp.minimum(source_of - 1, bound - receiver)
    moved = jax.random.randint(jax.random.fold_in(own_key, 1), (twos,), 0, 1 << 20) % (room + 1)
    tallies = tallies.at[1:1 + 2 * twos:2].set(source_of - moved).at[2:2 + 2 * twos:2].set(receiver + moved)
    return tallies[jax.random.permutation(jax.random.fold_in(own_key, 2), count)]


def gaussian(stream_key, dims, scale, limit, split=(), dtype=jnp.bfloat16):
    array = jax.random.normal(stream_key, dims, jnp.float32) * scale
    if len(split) > 0:
        array = block_scale(stream_key, dims, split, -0.22, 0.18) * array
    return jnp.clip(array, min=-limit, max=limit).astype(dtype)


def setup_inputs(seed: int = 0) -> dict:
    splits = jax.random.split(jax.random.key(seed), 12)
    states = gaussian(splits[0], (TOKENS, D), 0.1, 1.5, ((0, 16), (1, 8)))
    doc_lengths = ragged(splits[1], SEQS, TOKENS, TOKENS // 2, 2).astype(jnp.int32)
    attn_gain = draw_attn_gain(jax.random.fold_in(splits[11], 71), 0)
    query_weight = gaussian(splits[3], (D, HEADS * HD), D ** -0.5, 0.09375, ((1, 8),))
    key_weight = gaussian(splits[4], (D, KV_HEADS * HD), D ** -0.5, 0.09375, ((1, 8),))
    value_weight = gaussian(splits[5], (D, KV_HEADS * HD), D ** -0.5, 0.09375, ((1, 8),))
    output_weight = gaussian(splits[6], (HEADS * HD, D), HD ** -0.5, 0.5, ((0, 8),))
    mlp_gain = jnp.clip(1.0 + 0.1 * jax.random.normal(splits[7], (D,), jnp.float32), 0.5, 1.5)
    gate_weight = gaussian(splits[8], (D, FF), D ** -0.5, 0.09375, ((0, 16), (1, 8)))
    up_weight = gaussian(splits[9], (D, FF), D ** -0.5, 0.09375, ((0, 16), (1, 8)))
    down_weight = gaussian(splits[10], (FF, D), FF ** -0.5, 0.0625, ((0, 8), (1, 16)))
    return dict(states=states, doc_lengths=doc_lengths, attn_gain=attn_gain, query_weight=query_weight, key_weight=key_weight, value_weight=value_weight, output_weight=output_weight, mlp_gain=mlp_gain, gate_weight=gate_weight, up_weight=up_weight, down_weight=down_weight)


EPS = 1e-05
THETA = 500000.0

def rms_norm(rows, gain):
    rows = rows.astype(jnp.float32)
    factor = lax.rsqrt(lax.optimization_barrier(jnp.mean(rows * rows, axis=-1, keepdims=True)) + EPS)
    return (rows * factor * gain.astype(jnp.float32)).astype(jnp.bfloat16)

def rotary(block, where):
    half = block.shape[-1] // 2
    freq = THETA ** (-2.0 * jnp.arange(half).astype(jnp.float32) / block.shape[-1])
    angle = where.astype(jnp.float32)[:, None] * freq[None, :]
    cosine = jnp.cos(angle)[:, None, :]
    sine = jnp.sin(angle)[:, None, :]
    first = block[..., :half]
    second = block[..., half:]
    return jnp.concatenate([first * cosine - second * sine, second * cosine + first * sine], axis=-1)

def doc_layout(spots, lengths):
    ends = jnp.cumsum(lengths).astype(jnp.int32)
    after = spots[:, None] >= ends[None, :]
    documents = lax.optimization_barrier(jnp.sum(after.astype(jnp.int32), axis=1)).astype(jnp.int32)
    begins = lax.optimization_barrier(jnp.sum(jnp.where(after, lengths[None, :], 0), axis=1)).astype(jnp.int32)
    return (documents, (spots - begins).astype(jnp.int32))

def reference(states, doc_lengths, attn_gain, query_weight, key_weight, value_weight, output_weight, mlp_gain, gate_weight, up_weight, down_weight):
    tokens = states.shape[0]
    spots = jnp.arange(tokens).astype(jnp.int32)
    documents, where = doc_layout(spots, doc_lengths)
    normed = rms_norm(states, attn_gain)
    query = jnp.dot(normed, query_weight, preferred_element_type=jnp.float32).reshape(tokens, HEADS, HD)
    query = rotary(query, where).astype(jnp.bfloat16)
    keys = jnp.dot(normed, key_weight, preferred_element_type=jnp.float32).reshape(tokens, KV_HEADS, HD)
    keys = rotary(keys, where).astype(jnp.bfloat16)
    values = jnp.dot(normed, value_weight, preferred_element_type=jnp.float32).astype(jnp.bfloat16).reshape(tokens, KV_HEADS, HD)
    allowed = (documents[:, None] == documents[None, :]) & (spots[None, :] <= spots[:, None])
    group = HEADS // KV_HEADS
    scale = HD ** (-0.5)

    def one_head(head):
        q_head = lax.dynamic_index_in_dim(query, head, 1, keepdims=False)
        k_head = lax.dynamic_index_in_dim(keys, head // group, 1, keepdims=False)
        v_head = lax.dynamic_index_in_dim(values, head // group, 1, keepdims=False)
        scores = jnp.dot(q_head, k_head.T, preferred_element_type=jnp.float32) * scale
        masked = jnp.where(allowed, scores, -1e+30)
        highest = lax.optimization_barrier(jnp.max(masked, axis=1, keepdims=True))
        weights = jnp.where(allowed, jnp.exp(masked - highest), 0.0)
        total = lax.optimization_barrier(jnp.sum(weights, axis=1, keepdims=True))
        summed = jnp.dot(weights.astype(jnp.bfloat16), v_head, preferred_element_type=jnp.float32)
        return (summed / total).astype(jnp.bfloat16)
    heads_out = lax.map(one_head, jnp.arange(HEADS).astype(jnp.int32))
    attended = jnp.transpose(heads_out, (1, 0, 2)).reshape(tokens, HEADS * HD)
    mixed = (states.astype(jnp.float32) + jnp.dot(attended, output_weight, preferred_element_type=jnp.float32)).astype(jnp.bfloat16)
    normed_mlp = rms_norm(mixed, mlp_gain)
    gate = jnp.dot(normed_mlp, gate_weight, preferred_element_type=jnp.float32)
    up = jnp.dot(normed_mlp, up_weight, preferred_element_type=jnp.float32)
    hidden = (jax.nn.silu(gate) * up).astype(jnp.bfloat16)
    return (mixed.astype(jnp.float32) + jnp.dot(hidden, down_weight, preferred_element_type=jnp.float32)).astype(jnp.bfloat16)
```

```python
import jax
import jax.numpy as jnp
from jax import lax
from jax.sharding import PartitionSpec as P

HD = 128


EPS = 1e-05
THETA = 500000.0


def joined_along(tiles, dim):
    tiles = jnp.moveaxis(tiles, 0, dim)
    dims = tiles.shape
    return tiles.reshape(*dims[:dim], dims[dim] * dims[dim + 1], *dims[dim + 2 :])


def sent_to_all(array, axis):
    devices = lax.axis_size(axis)
    return lax.all_to_all(
        jnp.broadcast_to(array[None], (devices, *array.shape)), axis, 0, 0, tiled=True
    )


def gathered_copies(array, axis, dim):
    return joined_along(sent_to_all(array, axis), dim)


def side_by_side(arrays, axis, dim, along):
    ends, at = ([], 0)
    for a in arrays[:-1]:
        at += a.shape[along]
        ends.append(at)
    both = jnp.concatenate(arrays, axis=along)
    return tuple(jnp.split(lax.all_gather(both, axis, axis=dim, tiled=True), ends, axis=along))


def split_up(array, dim, devices):
    before, after = (array.shape[:dim], array.shape[dim + 1 :])
    return jnp.moveaxis(array.reshape(*before, devices, -1, *after), dim, 0)


def sum_at_owner(array, axis, dim):
    devices = lax.axis_size(axis)
    tiles = lax.all_to_all(
        split_up(array.astype(jnp.bfloat16), dim, devices), axis, 0, 0, tiled=True
    )
    return jnp.sum(tiles.astype(jnp.float32), axis=0)


def rms_norm(rows, gain):
    rows = rows.astype(jnp.float32)
    factor = lax.rsqrt(jnp.mean(rows * rows, axis=-1, keepdims=True) + EPS)
    return (rows * factor * gain).astype(jnp.bfloat16)


def rotary(block, where):
    half = block.shape[-1] // 2
    freq = THETA ** (-2.0 * jnp.arange(half).astype(jnp.float32) / block.shape[-1])
    angle = where.astype(jnp.float32)[:, None] * freq[None, :]
    cosine = jnp.cos(angle)[:, None, :]
    sine = jnp.sin(angle)[:, None, :]
    first = block[..., :half]
    second = block[..., half:]
    return jnp.concatenate(
        [first * cosine - second * sine, second * cosine + first * sine], axis=-1
    )


def doc_of(spots, ends):
    return jnp.sum((spots[:, None] >= ends[None, :]).astype(jnp.int32), axis=1)


def per_device(
    states,
    doc_lengths,
    attn_gain,
    query_weight,
    key_weight,
    value_weight,
    output_weight,
    mlp_gain,
    gate_weight,
    up_weight,
    down_weight,
):
    tok_rows = states.shape[0]
    head_dim = HD
    kv_local = key_weight.shape[1] // head_dim
    q_local = query_weight.shape[1] // head_dim
    group = q_local // kv_local
    scale = HD ** (-0.5)
    ends = jnp.cumsum(doc_lengths)
    own_rows = lax.axis_index("seq") * tok_rows + jnp.arange(tok_rows)
    after = own_rows[:, None] >= ends[None, :]
    where = own_rows - jnp.sum(jnp.where(after, doc_lengths[None, :], 0), axis=1)
    full_rows = gathered_copies(states, "tp", 1)
    normed = rms_norm(full_rows, attn_gain)
    query = jnp.dot(normed, query_weight, preferred_element_type=jnp.float32).reshape(
        tok_rows, q_local, head_dim
    )
    query = rotary(query, where).astype(jnp.bfloat16).reshape(tok_rows, q_local * head_dim)
    keys = jnp.dot(normed, key_weight, preferred_element_type=jnp.float32).reshape(
        tok_rows, kv_local, head_dim
    )
    keys = rotary(keys, where).astype(jnp.bfloat16).reshape(tok_rows, kv_local * head_dim)
    values = jnp.dot(normed, value_weight, preferred_element_type=jnp.float32).astype(jnp.bfloat16)
    query_docs = doc_of(own_rows, ends)
    query_heads = query.reshape(tok_rows, kv_local, group, head_dim)
    start_high = jnp.full((kv_local, group, tok_rows), -1e30, jnp.float32)
    start_total = jnp.zeros((kv_local, group, tok_rows), jnp.float32)
    start_summed = jnp.zeros((kv_local, group, tok_rows, head_dim), jnp.float32)
    both = gathered_copies(jnp.concatenate([keys, values], axis=1), "seq", 0)
    key_piece, value_piece = jnp.split(both, 2, axis=1)
    count = key_piece.shape[0]
    key_rows = jnp.arange(count)
    allowed = (query_docs[:, None] == doc_of(key_rows, ends)[None, :]) & (
        key_rows[None, :] <= own_rows[:, None]
    )

    def visit(state):
        highest, total, summed = state
        scores = (
            jnp.einsum(
                "rgad,sgd->gars",
                query_heads,
                key_piece.reshape(count, kv_local, head_dim),
                preferred_element_type=jnp.float32,
            )
            * scale
        )
        masked = jnp.where(allowed, scores, -1e30)
        new_high = jnp.maximum(highest, jnp.max(masked, axis=-1))
        weights = jnp.where(allowed, jnp.exp(masked - new_high[..., None]), 0.0)
        total = jnp.sum(weights, axis=-1)
        summed = jnp.einsum(
            "gars,sgd->gard",
            weights.astype(jnp.bfloat16),
            value_piece.reshape(count, kv_local, head_dim),
            preferred_element_type=jnp.float32,
        )
        return (new_high, total, summed)

    def skipped(state):
        return state

    highest, total, summed = lax.cond(
        jnp.any(allowed), visit, skipped, (start_high, start_total, start_summed)
    )
    attended = (summed / total[..., None]).astype(jnp.bfloat16)
    attended = jnp.transpose(attended, (2, 0, 1, 3)).reshape(tok_rows, q_local * head_dim)
    partial_value = jnp.dot(attended, output_weight, preferred_element_type=jnp.float32)
    shares = sum_at_owner(partial_value, "tp", 1)
    mixed = (states.astype(jnp.float32) + shares).astype(jnp.bfloat16)
    full_mixed = gathered_copies(mixed, "tp", 1)
    normed_mlp = rms_norm(full_mixed, mlp_gain)
    pieces = side_by_side((gate_weight, up_weight), "seq", 0, 1)
    gate = jnp.dot(normed_mlp, pieces[0], preferred_element_type=jnp.float32)
    up = jnp.dot(normed_mlp, pieces[1], preferred_element_type=jnp.float32)
    hidden = (jax.nn.silu(gate) * up).astype(jnp.bfloat16)
    terms = jnp.dot(
        hidden,
        lax.all_gather(down_weight, "seq", axis=1, tiled=True),
        preferred_element_type=jnp.float32,
    )
    shares_mlp = sum_at_owner(terms, "tp", 1)
    return (mixed.astype(jnp.float32) + shares_mlp).astype(jnp.bfloat16)


def solution(mesh):
    in_specs = (
        P("seq", "tp"),
        P(),
        P(),
        P(None, "tp"),
        P(None, "tp"),
        P(None, "tp"),
        P("tp", None),
        P(),
        P("seq", "tp"),
        P("seq", "tp"),
        P("tp", "seq"),
    )
    out_specs = P("seq", "tp")
    return jax.shard_map(
        per_device, mesh=mesh, in_specs=in_specs, out_specs=out_specs, check_vma=False
    )
```

```python
import functools

import jax
import jax.numpy as jnp
from jax import lax
from jax.experimental import pallas as pl
from jax.experimental.pallas import tpu as pltpu
from jax.sharding import PartitionSpec as P

HD = 128
EPS = 1e-05
THETA = 500000.0
MESH = pl.DeviceIdType.MESH
F32 = jnp.float32
BF16 = jnp.bfloat16
VM = pl.BlockSpec(memory_space=pltpu.VMEM)
ANY = pl.BlockSpec(memory_space=pl.ANY)


class Tp:
    def __init__(self):
        me = lax.axis_index("tp")
        y, z = me % 4, me // 4
        o = 1 - z
        self.me = me
        self.yp, self.ym, self.y2 = (z * 4 + (y + k) % 4 for k in (1, 3, 2))
        self.zz = o * 4 + y
        self.zyp, self.zym, self.zy2 = (o * 4 + (y + k) % 4 for k in (1, 3, 2))


class Seq:
    def __init__(self):
        me = lax.axis_index("seq")
        x, h, c = me // 4, (me // 2) % 2, me % 2
        g = 1 - h
        self.me = me
        self.xp, self.xm, self.x2 = (((x + k) % 4) * 4 + h * 2 + c for k in (1, 3, 2))
        self.hh = x * 4 + g * 2 + c
        self.hxp, self.hxm, self.hx2 = (((x + k) % 4) * 4 + g * 2 + c for k in (1, 3, 2))
        self.co = x * 4 + h * 2 + (1 - c)


def sender(axis, send, recv):
    def copy(at, src, dst, to):
        made = pltpu.make_async_remote_copy(
            src_ref=src,
            dst_ref=dst,
            send_sem=send.at[at],
            recv_sem=recv.at[at],
            device_id={axis: to},
            device_id_type=MESH,
        )
        made.start()
        return made

    return copy


def greet(tp, seq):
    barrier = pltpu.get_barrier_semaphore()
    near = [("tp", t) for t in (tp.yp, tp.ym, tp.zz)]
    if seq is not None:
        near += [("seq", s) for s in (seq.xp, seq.xm, seq.hh, seq.co)]
    for axis, to in near:
        pl.semaphore_signal(barrier, inc=1, device_id={axis: to}, device_id_type=MESH)
    pl.semaphore_wait(barrier, len(near))


def tp_gather(tp, own, buf, copy):
    half = own.shape[0] // 2
    lo, hi = pl.ds(0, half), pl.ds(half, half)
    a = copy(0, own, buf.at[tp.me], tp.yp)
    b = copy(1, own, buf.at[tp.me], tp.ym)
    c = copy(2, own, buf.at[tp.me], tp.zz)
    a.wait_recv()
    d = copy(3, buf.at[tp.ym, lo], buf.at[tp.ym, lo], tp.yp)
    b.wait_recv()
    e = copy(4, buf.at[tp.yp, hi], buf.at[tp.yp, hi], tp.ym)
    c.wait_recv()
    f = copy(5, buf.at[tp.zz], buf.at[tp.zz], tp.yp)
    g = copy(6, buf.at[tp.zz], buf.at[tp.zz], tp.ym)
    d.wait_recv()
    h = copy(7, buf.at[tp.y2, lo], buf.at[tp.y2, lo], tp.zz)
    e.wait_recv()
    i = copy(8, buf.at[tp.y2, hi], buf.at[tp.y2, hi], tp.zz)
    for one in (f, g, h, i):
        one.wait_recv()
    for one in (a, b, c, d, e, f, g, h, i):
        one.wait_send()


def add_to(ref, *others):
    total = ref[...].astype(F32)
    for other in others:
        total = total + other[...].astype(F32)
    ref[...] = total.astype(ref.dtype)


def tp_sum(tp, fill, part, ra, rb, rc, rd, re, copy):
    half = ra.shape[0] // 2
    lo, hi = pl.ds(0, half), pl.ds(half, half)
    fill(tp.zy2)
    a = copy(0, part.at[tp.zy2], ra, tp.zz)
    fill(tp.zyp)
    b = copy(1, part.at[tp.zyp], rc.at[0], tp.yp)
    fill(tp.zym)
    c = copy(2, part.at[tp.zym], rc.at[1], tp.ym)
    fill(tp.y2)
    fill(tp.zz)
    fill(tp.yp)
    fill(tp.ym)
    fill(tp.me)
    a.wait_recv()
    add_to(part.at[tp.y2], ra)
    d = copy(3, part.at[tp.y2, lo], rb.at[0], tp.ym)
    e = copy(4, part.at[tp.y2, hi], rb.at[1], tp.yp)
    b.wait_recv()
    c.wait_recv()
    add_to(part.at[tp.zz], rc.at[0], rc.at[1])
    f = copy(5, part.at[tp.zz], rd, tp.zz)
    d.wait_recv()
    add_to(part.at[tp.ym, lo], rb.at[0])
    g = copy(6, part.at[tp.ym], re.at[0], tp.ym)
    e.wait_recv()
    add_to(part.at[tp.yp, hi], rb.at[1])
    h = copy(7, part.at[tp.yp], re.at[1], tp.yp)
    for one in (f, g, h):
        one.wait_recv()
    total = part[tp.me].astype(F32) + rd[...].astype(F32)
    total = total + re[0].astype(F32) + re[1].astype(F32)
    for one in (a, b, c, d, e, f, g, h):
        one.wait_send()
    return total


def seq_gather(seq, buf, copy, copy_in):
    half = buf.shape[1] // 2
    lo, hi = pl.ds(0, half), pl.ds(half, half)
    sent, inner = [], []

    def pass_on(at, ref, to):
        sent.append(copy(at, ref, ref, to))
        return sent[-1]

    def share(ref):
        inner.append(copy_in(len(inner), ref, ref, seq.co))

    own = buf.at[seq.me]
    c = pass_on(2, own, seq.hh)
    a = pass_on(0, own, seq.xp)
    b = pass_on(1, own, seq.xm)
    share(own)
    a.wait_recv()
    d = pass_on(3, buf.at[seq.xm, lo], seq.xp)
    share(buf.at[seq.xm])
    b.wait_recv()
    e = pass_on(4, buf.at[seq.xp, hi], seq.xm)
    share(buf.at[seq.xp])
    c.wait_recv()
    f = pass_on(5, buf.at[seq.hh], seq.xp)
    g = pass_on(6, buf.at[seq.hh], seq.xm)
    share(buf.at[seq.hh])
    d.wait_recv()
    share(buf.at[seq.x2, lo])
    e.wait_recv()
    share(buf.at[seq.x2, hi])
    f.wait_recv()
    h = pass_on(7, buf.at[seq.hxm, lo], seq.xp)
    share(buf.at[seq.hxm])
    g.wait_recv()
    i = pass_on(8, buf.at[seq.hxp, hi], seq.xm)
    share(buf.at[seq.hxp])
    h.wait_recv()
    share(buf.at[seq.hx2, lo])
    i.wait_recv()
    share(buf.at[seq.hx2, hi])
    for one in inner:
        one.wait_recv()
    for one in sent + inner:
        one.wait_send()


def norm_factor(buf):
    blocks, rows, wide = buf.shape

    def add(t, squares):
        block = buf[t].astype(F32)
        return squares + jnp.sum(block * block, axis=-1, keepdims=True)

    squares = lax.fori_loop(0, blocks, add, jnp.zeros((rows, 1), F32))
    return lax.rsqrt(squares / (blocks * wide) + EPS)


def turned(block, cosine, sine):
    return block * cosine + pltpu.roll(block, HD // 2, 1) * sine


def attention_kernel(
    states,
    begins,
    cosine,
    sine,
    gain,
    mlp_gain,
    wq_hbm,
    wk_hbm,
    wv_hbm,
    wo_hbm,
    mixed,
    normed_mlp,
    rows_all,
    wq,
    wk,
    wv,
    wo,
    qacc,
    kvacc,
    kv,
    query,
    scores,
    best,
    totals,
    attended,
    part,
    ra,
    rb,
    rc,
    rd,
    re,
    mixed_all,
    load,
    s1,
    r1,
    s2,
    r2,
    s3,
    r3,
    s4,
    r4,
    s5,
    r5,
):
    tp, seq = Tp(), Seq()
    tok, wide = states.shape
    heads = wq.shape[1] // HD
    loads = [
        pltpu.make_async_copy(a, b, load.at[i])
        for i, (a, b) in enumerate(((wq_hbm, wq), (wk_hbm, wk), (wv_hbm, wv), (wo_hbm, wo)))
    ]
    for one in loads:
        one.start()
    greet(tp, seq)
    rows_all[tp.me] = states[...]
    tp_gather(tp, states, rows_all, sender("tp", s1, r1))
    factor = norm_factor(rows_all)
    qacc[...] = jnp.zeros_like(qacc)
    kvacc[...] = jnp.zeros_like(kvacc)
    for one in loads[:3]:
        one.wait()

    def project(t, carry):
        normed = (rows_all[t].astype(F32) * factor * gain[t]).astype(BF16)
        at = pl.ds(pl.multiple_of(t * wide, wide), wide)
        qacc[...] += jnp.dot(normed, wq[at, :], preferred_element_type=F32)
        kvacc[:, :HD] += jnp.dot(normed, wk[at, :], preferred_element_type=F32)
        kvacc[:, HD:] += jnp.dot(normed, wv[at, :], preferred_element_type=F32)
        return carry

    lax.fori_loop(0, rows_all.shape[0], project, 0)
    kv[seq.me, :, :HD] = turned(kvacc[:, :HD], cosine[...], sine[...]).astype(BF16)
    kv[seq.me, :, HD:] = kvacc[:, HD:].astype(BF16)
    for h in range(heads):
        block = qacc[:, h * HD : (h + 1) * HD]
        query[h] = turned(block, cosine[...], sine[...]).astype(BF16)
    seq_gather(seq, kv, sender("seq", s2, r2), sender("seq", s3, r3))

    blocks = scores.shape[0]
    slots = kv.shape[0]
    best[...] = jnp.full_like(best, -1e30)
    totals[...] = jnp.zeros_like(totals)

    def score(j, carry):
        keys = kv[(seq.me + slots - j) % slots, :, :HD]
        cols = lax.broadcasted_iota(jnp.int32, (tok, tok), 1) + (seq.me - j) * tok
        lines = lax.broadcasted_iota(jnp.int32, (tok, tok), 0) + seq.me * tok
        allowed = (cols >= begins[...]) & (cols <= lines)
        for h in range(heads):
            found = lax.dot_general(
                query[h], keys, (((1,), (1,)), ((), ())), preferred_element_type=F32
            )
            masked = jnp.where(allowed, found * HD ** (-0.5), -1e30)
            scores[j, h] = masked
            best[h] = jnp.maximum(best[h], masked)
        return carry

    lax.fori_loop(0, blocks, score, 0)
    qacc[...] = jnp.zeros_like(qacc)
    highest = [jnp.max(best[h], axis=-1, keepdims=True) for h in range(heads)]
    for h in range(heads):
        best[h] = jnp.broadcast_to(highest[h], (tok, tok))

    def weigh(j, carry):
        values = kv[(seq.me + slots - j) % slots, :, HD:]
        for h in range(heads):
            weights = jnp.exp(scores[j, h] - best[h])
            totals[h] += weights
            qacc[:, h * HD : (h + 1) * HD] += jnp.dot(
                weights.astype(BF16), values, preferred_element_type=F32
            )
        return carry

    lax.fori_loop(0, blocks, weigh, 0)
    for h in range(heads):
        at = slice(h * HD, (h + 1) * HD)
        total = jnp.sum(totals[h], axis=-1, keepdims=True)
        attended[:, at] = (qacc[:, at] / total).astype(BF16)
    loads[3].wait()

    def fill(slot):
        at = pl.ds(pl.multiple_of(slot * wide, wide), wide)
        part[slot] = jnp.dot(attended[...], wo[:, at], preferred_element_type=F32).astype(BF16)

    shares = tp_sum(tp, fill, part, ra, rb, rc, rd, re, sender("tp", s4, r4))
    own = (states[...].astype(F32) + shares).astype(BF16)
    mixed[...] = own
    mixed_all[tp.me] = own
    tp_gather(tp, mixed, mixed_all, sender("tp", s5, r5))
    factor = norm_factor(mixed_all)
    for t in range(mixed_all.shape[0]):
        normed_mlp[:, t * wide : (t + 1) * wide] = (
            mixed_all[t].astype(F32) * factor * mlp_gain[t]
        ).astype(BF16)


def down_kernel(
    hidden, mixed, down_hbm, out, down, part, ra, rb, rc, rd, re, load, send, recv
):
    tp = Tp()
    wide = mixed.shape[1]
    order = (tp.zy2, tp.zyp, tp.zym, tp.y2, tp.zz, tp.yp, tp.ym, tp.me)
    loads = []
    for i, slot in enumerate(order):
        at = pl.ds(pl.multiple_of(slot * wide, wide), wide)
        loads.append(pltpu.make_async_copy(down_hbm.at[:, at], down.at[slot], load.at[i]))
        loads[-1].start()
    greet(tp, None)
    waiting = iter(loads)

    def fill(slot):
        next(waiting).wait()
        part[slot] = jnp.dot(hidden[...], down[slot], preferred_element_type=F32).astype(BF16)

    shares = tp_sum(tp, fill, part, ra, rb, rc, rd, re, sender("tp", send, recv))
    out[...] = (mixed[...].astype(F32) + shares).astype(BF16)


def sum_scratch(tps, tok, wide):
    return [
        pltpu.VMEM((tps, tok, wide), BF16),
        pltpu.VMEM((tok, wide), BF16),
        pltpu.VMEM((2, tok // 2, wide), BF16),
        pltpu.VMEM((2, tok, wide), BF16),
        pltpu.VMEM((tok, wide), BF16),
        pltpu.VMEM((2, tok, wide), BF16),
    ]


def dma(*counts):
    return [pltpu.SemaphoreType.DMA((n,)) for n in counts]


def per_device(
    states,
    doc_lengths,
    attn_gain,
    query_weight,
    key_weight,
    value_weight,
    output_weight,
    mlp_gain,
    gate_weight,
    up_weight,
    down_weight,
):
    tok, wide = states.shape
    tps, seqs = lax.axis_size("tp"), lax.axis_size("seq")
    heads = query_weight.shape[1] // HD
    spots = lax.axis_index("seq") * tok + jnp.arange(tok)
    after = spots[:, None] >= jnp.cumsum(doc_lengths)[None, :]
    begins = jnp.sum(jnp.where(after, doc_lengths[None, :], 0), axis=1)
    half = HD // 2
    freq = THETA ** (-2.0 * jnp.arange(half).astype(F32) / HD)
    angle = (spots - begins).astype(F32)[:, None] * freq[None, :]
    cos, sin = jnp.cos(angle), jnp.sin(angle)
    cosine = jnp.concatenate([cos, cos], axis=1)
    sine = jnp.concatenate([-sin, sin], axis=1)
    blocks = min(seqs, 2048 // tok + 1)

    rows = lax.all_gather(
        jnp.concatenate([gate_weight, up_weight], axis=1), "seq", axis=0, tiled=True
    )
    down = lax.all_gather(down_weight, "seq", axis=1, tiled=True)

    mixed, normed_mlp = pl.pallas_call(
        attention_kernel,
        out_shape=(
            jax.ShapeDtypeStruct((tok, wide), BF16),
            jax.ShapeDtypeStruct((tok, tps * wide), BF16),
        ),
        in_specs=[VM] * 6 + [ANY] * 4,
        out_specs=(VM, VM),
        scratch_shapes=[
            pltpu.VMEM((tps, tok, wide), BF16),
            pltpu.VMEM(query_weight.shape, BF16),
            pltpu.VMEM(key_weight.shape, BF16),
            pltpu.VMEM(value_weight.shape, BF16),
            pltpu.VMEM(output_weight.shape, BF16),
            pltpu.VMEM((tok, heads * HD), F32),
            pltpu.VMEM((tok, 2 * HD), F32),
            pltpu.VMEM((seqs, tok, 2 * HD), BF16),
            pltpu.VMEM((heads, tok, HD), BF16),
            pltpu.VMEM((blocks, heads, tok, tok), F32),
            pltpu.VMEM((heads, tok, tok), F32),
            pltpu.VMEM((heads, tok, tok), F32),
            pltpu.VMEM((tok, heads * HD), BF16),
            *sum_scratch(tps, tok, wide),
            pltpu.VMEM((tps, tok, wide), BF16),
            *dma(4, 9, 9, 9, 9, 10, 10, 8, 8, 9, 9),
        ],
        compiler_params=pltpu.CompilerParams(
            collective_id=0, has_side_effects=True, vmem_limit_bytes=60 * 1024 * 1024
        ),
        cost_estimate=pl.CostEstimate(
            flops=6 * 10**10, bytes_accessed=2 * 10**7, transcendentals=2 * 10**6
        ),
        name="attention",
    )(
        states,
        begins.astype(jnp.int32)[:, None],
        cosine,
        sine,
        attn_gain.reshape(tps, 1, wide),
        mlp_gain.reshape(tps, 1, wide),
        query_weight,
        key_weight,
        value_weight,
        output_weight,
    )
    both = jnp.dot(normed_mlp, rows, preferred_element_type=F32)
    gate, up = jnp.split(both, 2, axis=1)
    hidden = (jax.nn.silu(gate) * up).astype(BF16)
    return pl.pallas_call(
        down_kernel,
        out_shape=jax.ShapeDtypeStruct((tok, wide), BF16),
        in_specs=[VM, VM, ANY],
        out_specs=VM,
        scratch_shapes=[
            pltpu.VMEM((tps, down.shape[0], wide), BF16),
            *sum_scratch(tps, tok, wide),
            *dma(8, 8, 8),
        ],
        compiler_params=pltpu.CompilerParams(
            collective_id=1, has_side_effects=True, vmem_limit_bytes=60 * 1024 * 1024
        ),
        cost_estimate=pl.CostEstimate(flops=10**10, bytes_accessed=10**7, transcendentals=0),
        name="down",
    )(hidden, mixed, down)


def solution(mesh):
    in_specs = (
        P("seq", "tp"),
        P(),
        P(),
        P(None, "tp"),
        P(None, "tp"),
        P(None, "tp"),
        P("tp", None),
        P(),
        P("seq", "tp"),
        P("seq", "tp"),
        P("tp", "seq"),
    )
    return jax.shard_map(
        per_device, mesh=mesh, in_specs=in_specs, out_specs=P("seq", "tp"), check_vma=False
    )
```

```python
import functools

import jax
import jax.numpy as jnp
from jax import lax
from jax.experimental import pallas as pl
from jax.experimental.pallas import tpu as pltpu
from jax.sharding import PartitionSpec as P

HD = 128
EPS = 1e-05
THETA = 500000.0
MESH = pl.DeviceIdType.MESH
F32 = jnp.float32
BF16 = jnp.bfloat16
VM = pl.BlockSpec(memory_space=pltpu.VMEM)
ANY = pl.BlockSpec(memory_space=pl.ANY)


class Tp:
    def __init__(self):
        me = lax.axis_index("tp")
        y, z = me % 4, me // 4
        o = 1 - z
        self.me = me
        self.yp, self.ym, self.y2 = (z * 4 + (y + k) % 4 for k in (1, 3, 2))
        self.zz = o * 4 + y
        self.zyp, self.zym, self.zy2 = (o * 4 + (y + k) % 4 for k in (1, 3, 2))


class Seq:
    def __init__(self):
        me = lax.axis_index("seq")
        x, h, c = me // 4, (me // 2) % 2, me % 2
        g = 1 - h
        self.me = me
        self.xp, self.xm, self.x2 = (((x + k) % 4) * 4 + h * 2 + c for k in (1, 3, 2))
        self.hh = x * 4 + g * 2 + c
        self.hxp, self.hxm, self.hx2 = (((x + k) % 4) * 4 + g * 2 + c for k in (1, 3, 2))
        self.co = x * 4 + h * 2 + (1 - c)


def sender(axis, send, recv):
    def copy(at, src, dst, to):
        made = pltpu.make_async_remote_copy(
            src_ref=src,
            dst_ref=dst,
            send_sem=send.at[at],
            recv_sem=recv.at[at],
            device_id={axis: to},
            device_id_type=MESH,
        )
        made.start()
        return made

    return copy


def greet(tp, seq):
    barrier = pltpu.get_barrier_semaphore()
    near = [("tp", t) for t in (tp.yp, tp.ym, tp.zz)]
    if seq is not None:
        near += [("seq", s) for s in (seq.xp, seq.xm, seq.hh, seq.co)]
    for axis, to in near:
        pl.semaphore_signal(barrier, inc=1, device_id={axis: to}, device_id_type=MESH)
    pl.semaphore_wait(barrier, len(near))


def tp_gather(tp, own, buf, copy, begun, by_z):
    half = own.shape[0] // 2
    lo, hi = pl.ds(0, half), pl.ds(half, half)
    sent = []

    def go(at, src, dst, to):
        sent.append(copy(at, src, dst, to))
        return sent[-1]

    c = go(2, own, buf.at[tp.me], tp.zz)
    a = go(0, own, buf.at[tp.me], tp.yp)
    b = go(1, own, buf.at[tp.me], tp.ym)
    begun()
    a.wait_recv()
    d = go(3, buf.at[tp.ym, lo], buf.at[tp.ym, lo], tp.yp)
    b.wait_recv()
    e = go(4, buf.at[tp.yp, hi], buf.at[tp.yp, hi], tp.ym)
    c.wait_recv()
    f = go(5, buf.at[tp.zz], buf.at[tp.zz], tp.yp)
    g = go(6, buf.at[tp.zz], buf.at[tp.zz], tp.ym)
    if by_z:
        d.wait_recv()
        h = go(7, buf.at[tp.y2, lo], buf.at[tp.y2, lo], tp.zz)
        e.wait_recv()
        i = go(8, buf.at[tp.y2, hi], buf.at[tp.y2, hi], tp.zz)
        f.wait_recv()
        g.wait_recv()
    else:
        f.wait_recv()
        h = go(7, buf.at[tp.zym, lo], buf.at[tp.zym, lo], tp.yp)
        g.wait_recv()
        i = go(8, buf.at[tp.zyp, hi], buf.at[tp.zyp, hi], tp.ym)
        d.wait_recv()
        e.wait_recv()
    h.wait_recv()
    i.wait_recv()
    for one in sent:
        one.wait_send()


def add_to(ref, *others):
    total = ref[...].astype(F32)
    for other in others:
        total = total + other[...].astype(F32)
    ref[...] = total.astype(ref.dtype)


def tp_sum(tp, fill, part, ra, rb, rc, rd, re, copy):
    half = ra.shape[0] // 2
    lo, hi = pl.ds(0, half), pl.ds(half, half)
    fill(tp.zy2)
    a = copy(0, part.at[tp.zy2], ra, tp.zz)
    fill(tp.zyp)
    b = copy(1, part.at[tp.zyp], rc.at[0], tp.yp)
    fill(tp.zym)
    c = copy(2, part.at[tp.zym], rc.at[1], tp.ym)
    fill(tp.y2)
    fill(tp.zz)
    fill(tp.yp)
    fill(tp.ym)
    fill(tp.me)
    a.wait_recv()
    add_to(part.at[tp.y2], ra)
    d = copy(3, part.at[tp.y2, lo], rb.at[0], tp.ym)
    e = copy(4, part.at[tp.y2, hi], rb.at[1], tp.yp)
    b.wait_recv()
    c.wait_recv()
    add_to(part.at[tp.zz], rc.at[0], rc.at[1])
    f = copy(5, part.at[tp.zz], rd, tp.zz)
    d.wait_recv()
    add_to(part.at[tp.ym, lo], rb.at[0])
    g = copy(6, part.at[tp.ym], re.at[0], tp.ym)
    e.wait_recv()
    add_to(part.at[tp.yp, hi], rb.at[1])
    h = copy(7, part.at[tp.yp], re.at[1], tp.yp)
    for one in (f, g, h):
        one.wait_recv()
    total = part[tp.me].astype(F32) + rd[...].astype(F32)
    total = total + re[0].astype(F32) + re[1].astype(F32)
    for one in (a, b, c, d, e, f, g, h):
        one.wait_send()
    return total


class SeqGather:
    def __init__(self, seq, buf, first, rows, copy, copy_in):
        self.seq, self.buf, self.copy, self.copy_in = seq, buf, copy, copy_in
        self.all = pl.ds(first, rows)
        self.lo, self.hi = pl.ds(first, rows // 2), pl.ds(first + rows // 2, rows // 2)
        self.sent, self.inner, self.by = [], [], {}

    def go(self, at, slot, rows, to):
        ref = self.buf.at[slot, rows]
        self.by[at] = self.copy(at, ref, ref, to)
        self.sent.append(self.by[at])

    def share(self, slot, rows):
        ref = self.buf.at[slot, rows]
        self.inner.append(self.copy_in(len(self.inner), ref, ref, self.seq.co))

    def start_x(self):
        q = self.seq
        self.go(0, q.me, self.all, q.xp)
        self.go(1, q.me, self.all, q.xm)
        self.share(q.me, self.all)

    def start_h(self):
        self.go(2, self.seq.me, self.all, self.seq.hh)

    def own_row(self):
        q = self.seq
        self.by[0].wait_recv()
        self.go(3, q.xm, self.lo, q.xp)
        self.share(q.xm, self.all)
        self.by[1].wait_recv()
        self.go(4, q.xp, self.hi, q.xm)
        self.share(q.xp, self.all)

    def other_row(self):
        q = self.seq
        self.by[2].wait_recv()
        self.go(5, q.hh, self.all, q.xp)
        self.go(6, q.hh, self.all, q.xm)
        self.share(q.hh, self.all)

    def far(self):
        q = self.seq
        self.by[5].wait_recv()
        self.go(7, q.hxm, self.lo, q.xp)
        self.share(q.hxm, self.all)
        self.by[6].wait_recv()
        self.go(8, q.hxp, self.hi, q.xm)
        self.share(q.hxp, self.all)
        self.by[3].wait_recv()
        self.share(q.x2, self.lo)
        self.by[4].wait_recv()
        self.share(q.x2, self.hi)

    def last(self):
        q = self.seq
        self.by[7].wait_recv()
        self.share(q.hx2, self.lo)
        self.by[8].wait_recv()
        self.share(q.hx2, self.hi)
        for one in self.inner:
            one.wait_recv()

    def sends_done(self):
        for one in self.sent + self.inner:
            one.wait_send()


def norm_factor(buf):
    blocks, rows, wide = buf.shape

    def add(t, squares):
        block = buf[t].astype(F32)
        return squares + jnp.sum(block * block, axis=-1, keepdims=True)

    squares = lax.fori_loop(0, blocks, add, jnp.zeros((rows, 1), F32))
    return lax.rsqrt(squares / (blocks * wide) + EPS)


def turned(block, cosine, sine):
    return block * cosine + pltpu.roll(block, HD // 2, 1) * sine


def attention_kernel(
    states,
    begins,
    cosine,
    sine,
    gain,
    mlp_gain,
    wq_hbm,
    wk_hbm,
    wv_hbm,
    wo_hbm,
    gate_hbm,
    up_hbm,
    mixed,
    hidden,
    rows_all,
    wq,
    wk,
    wv,
    wo,
    qacc,
    kvacc,
    kv,
    query,
    scores,
    best,
    totals,
    attended,
    part,
    ra,
    rb,
    rc,
    rd,
    re,
    mixed_all,
    normed_mlp,
    ff,
    ffacc,
    load,
    s1,
    r1,
    s2,
    r2,
    s3,
    r3,
    s4,
    r4,
    s5,
    r5,
    s6,
    r6,
    s7,
    r7,
):
    tp, seq = Tp(), Seq()
    tok, wide = states.shape
    heads = wq.shape[1] // HD
    units = gate_hbm.shape[1]
    moves = (
        (gate_hbm, ff.at[seq.me, :, :units]),
        (up_hbm, ff.at[seq.me, :, units:]),
        (wq_hbm, wq),
        (wk_hbm, wk),
        (wv_hbm, wv),
        (wo_hbm, wo),
    )
    loads = [pltpu.make_async_copy(a, b, load.at[i]) for i, (a, b) in enumerate(moves)]
    for one in loads:
        one.start()
    chunks = s6.shape[0]
    deep = gate_hbm.shape[0] // chunks
    weights = [
        SeqGather(
            seq,
            ff,
            i * deep,
            deep,
            sender("seq", s6.at[i], r6.at[i]),
            sender("seq", s7.at[i], r7.at[i]),
        )
        for i in range(chunks)
    ]
    greet(tp, seq)

    def begun():
        loads[0].wait()
        loads[1].wait()
        weights[0].start_x()
        weights[0].start_h()
        weights[1].start_x()
        rows_all[tp.me] = states[...]

    tp_gather(tp, states, rows_all, sender("tp", s1, r1), begun, False)
    weights[0].own_row()
    factor = norm_factor(rows_all)
    qacc[...] = jnp.zeros_like(qacc)
    kvacc[...] = jnp.zeros_like(kvacc)
    for one in loads[2:5]:
        one.wait()

    def project(t, carry):
        normed = (rows_all[t].astype(F32) * factor * gain[t]).astype(BF16)
        at = pl.ds(pl.multiple_of(t * wide, wide), wide)
        qacc[...] += jnp.dot(normed, wq[at, :], preferred_element_type=F32)
        kvacc[:, :HD] += jnp.dot(normed, wk[at, :], preferred_element_type=F32)
        kvacc[:, HD:] += jnp.dot(normed, wv[at, :], preferred_element_type=F32)
        return carry

    lax.fori_loop(0, rows_all.shape[0], project, 0)
    kv[seq.me, :, :HD] = turned(kvacc[:, :HD], cosine[...], sine[...]).astype(BF16)
    kv[seq.me, :, HD:] = kvacc[:, HD:].astype(BF16)
    for h in range(heads):
        block = qacc[:, h * HD : (h + 1) * HD]
        query[h] = turned(block, cosine[...], sine[...]).astype(BF16)
    keys_values = SeqGather(seq, kv, 0, tok, sender("seq", s2, r2), sender("seq", s3, r3))
    keys_values.start_h()
    keys_values.start_x()
    weights[1].start_h()
    keys_values.own_row()
    keys_values.other_row()
    keys_values.far()
    keys_values.last()
    weights[1].own_row()
    weights[0].other_row()

    blocks = scores.shape[0]
    slots = kv.shape[0]
    best[...] = jnp.full_like(best, -1e30)
    totals[...] = jnp.zeros_like(totals)

    def score(j, carry):
        keys = kv[(seq.me + slots - j) % slots, :, :HD]
        cols = lax.broadcasted_iota(jnp.int32, (tok, tok), 1) + (seq.me - j) * tok
        lines = lax.broadcasted_iota(jnp.int32, (tok, tok), 0) + seq.me * tok
        allowed = (cols >= begins[...]) & (cols <= lines)
        for h in range(heads):
            found = lax.dot_general(
                query[h], keys, (((1,), (1,)), ((), ())), preferred_element_type=F32
            )
            masked = jnp.where(allowed, found * HD ** (-0.5), -1e30)
            scores[j, h] = masked
            best[h] = jnp.maximum(best[h], masked)
        return carry

    lax.fori_loop(0, blocks, score, 0)
    weights[0].far()
    weights[1].other_row()
    qacc[...] = jnp.zeros_like(qacc)
    highest = [jnp.max(best[h], axis=-1, keepdims=True) for h in range(heads)]
    for h in range(heads):
        best[h] = jnp.broadcast_to(highest[h], (tok, tok))

    def weigh(j, carry):
        values = kv[(seq.me + slots - j) % slots, :, HD:]
        for h in range(heads):
            shares = jnp.exp(scores[j, h] - best[h])
            totals[h] += shares
            qacc[:, h * HD : (h + 1) * HD] += jnp.dot(
                shares.astype(BF16), values, preferred_element_type=F32
            )
        return carry

    lax.fori_loop(0, blocks, weigh, 0)
    for h in range(heads):
        at = slice(h * HD, (h + 1) * HD)
        total = jnp.sum(totals[h], axis=-1, keepdims=True)
        attended[:, at] = (qacc[:, at] / total).astype(BF16)
    loads[5].wait()

    def fill(slot):
        at = pl.ds(pl.multiple_of(slot * wide, wide), wide)
        part[slot] = jnp.dot(attended[...], wo[:, at], preferred_element_type=F32).astype(BF16)

    shares = tp_sum(tp, fill, part, ra, rb, rc, rd, re, sender("tp", s4, r4))
    weights[1].far()
    own = (states[...].astype(F32) + shares).astype(BF16)
    mixed[...] = own
    mixed_all[tp.me] = own
    tp_gather(tp, mixed, mixed_all, sender("tp", s5, r5), lambda: None, True)
    factor = norm_factor(mixed_all)
    cut = normed_mlp.shape[2]
    for s in range(normed_mlp.shape[0]):
        at = pl.ds(s * cut % wide, cut)
        block = mixed_all[s * cut // wide, :, at].astype(F32)
        normed_mlp[s] = (block * factor * mlp_gain[s]).astype(BF16)
    for one in weights:
        one.last()
    ffacc[...] = jnp.zeros_like(ffacc)

    def feed(s, carry):
        for at in (pl.ds(0, units), pl.ds(units, units)):
            terms = ffacc[:, at]
            for k in range(4):
                terms += jnp.dot(
                    normed_mlp[s * 4 + k], ff[s * 4 + k, :, at], preferred_element_type=F32
                )
            ffacc[:, at] = terms
        return carry

    lax.fori_loop(0, normed_mlp.shape[0] // 4, feed, 0)
    gate = ffacc[:, :units]
    hidden[...] = (gate / (1.0 + jnp.exp(-gate)) * ffacc[:, units:]).astype(BF16)
    for one in [keys_values] + weights:
        one.sends_done()


def down_kernel(
    hidden, mixed, down_hbm, out, down, part, ra, rb, rc, rd, re, load, send, recv
):
    tp = Tp()
    wide = mixed.shape[1]
    order = (tp.zy2, tp.zyp, tp.zym, tp.y2, tp.zz, tp.yp, tp.ym, tp.me)
    loads = []
    for i, slot in enumerate(order):
        at = pl.ds(pl.multiple_of(slot * wide, wide), wide)
        loads.append(pltpu.make_async_copy(down_hbm.at[:, at], down.at[slot], load.at[i]))
        loads[-1].start()
    greet(tp, None)
    waiting = iter(loads)

    def fill(slot):
        next(waiting).wait()
        part[slot] = jnp.dot(hidden[...], down[slot], preferred_element_type=F32).astype(BF16)

    shares = tp_sum(tp, fill, part, ra, rb, rc, rd, re, sender("tp", send, recv))
    out[...] = (mixed[...].astype(F32) + shares).astype(BF16)


def sum_scratch(tps, tok, wide):
    return [
        pltpu.VMEM((tps, tok, wide), BF16),
        pltpu.VMEM((tok, wide), BF16),
        pltpu.VMEM((2, tok // 2, wide), BF16),
        pltpu.VMEM((2, tok, wide), BF16),
        pltpu.VMEM((tok, wide), BF16),
        pltpu.VMEM((2, tok, wide), BF16),
    ]


def dma(*counts):
    return [pltpu.SemaphoreType.DMA((n,)) for n in counts]


def per_device(
    states,
    doc_lengths,
    attn_gain,
    query_weight,
    key_weight,
    value_weight,
    output_weight,
    mlp_gain,
    gate_weight,
    up_weight,
    down_weight,
):
    tok, wide = states.shape
    tps, seqs = lax.axis_size("tp"), lax.axis_size("seq")
    heads = query_weight.shape[1] // HD
    depth, units = gate_weight.shape
    spots = lax.axis_index("seq") * tok + jnp.arange(tok)
    after = spots[:, None] >= jnp.cumsum(doc_lengths)[None, :]
    begins = jnp.sum(jnp.where(after, doc_lengths[None, :], 0), axis=1)
    half = HD // 2
    freq = THETA ** (-2.0 * jnp.arange(half).astype(F32) / HD)
    angle = (spots - begins).astype(F32)[:, None] * freq[None, :]
    cos, sin = jnp.cos(angle), jnp.sin(angle)
    cosine = jnp.concatenate([cos, cos], axis=1)
    sine = jnp.concatenate([-sin, sin], axis=1)
    blocks = min(seqs, 2048 // tok + 1)

    down = lax.all_gather(down_weight, "seq", axis=1, tiled=True)

    mixed, hidden = pl.pallas_call(
        attention_kernel,
        out_shape=(
            jax.ShapeDtypeStruct((tok, wide), BF16),
            jax.ShapeDtypeStruct((tok, units), BF16),
        ),
        in_specs=[VM] * 6 + [ANY] * 6,
        out_specs=(VM, VM),
        scratch_shapes=[
            pltpu.VMEM((tps, tok, wide), BF16),
            pltpu.VMEM(query_weight.shape, BF16),
            pltpu.VMEM(key_weight.shape, BF16),
            pltpu.VMEM(value_weight.shape, BF16),
            pltpu.VMEM(output_weight.shape, BF16),
            pltpu.VMEM((tok, heads * HD), F32),
            pltpu.VMEM((tok, 2 * HD), F32),
            pltpu.VMEM((seqs, tok, 2 * HD), BF16),
            pltpu.VMEM((heads, tok, HD), BF16),
            pltpu.VMEM((blocks, heads, tok, tok), F32),
            pltpu.VMEM((heads, tok, tok), F32),
            pltpu.VMEM((heads, tok, tok), F32),
            pltpu.VMEM((tok, heads * HD), BF16),
            *sum_scratch(tps, tok, wide),
            pltpu.VMEM((tps, tok, wide), BF16),
            pltpu.VMEM((seqs, tok, depth), BF16),
            pltpu.VMEM((seqs, depth, 2 * units), BF16),
            pltpu.VMEM((tok, 2 * units), F32),
            *dma(6, 9, 9, 9, 9, 10, 10, 8, 8, 9, 9),
            *[pltpu.SemaphoreType.DMA((2, n)) for n in (9, 9, 10, 10)],
        ],
        compiler_params=pltpu.CompilerParams(
            collective_id=0, has_side_effects=True, vmem_limit_bytes=60 * 1024 * 1024
        ),
        cost_estimate=pl.CostEstimate(
            flops=6 * 10**10, bytes_accessed=2 * 10**7, transcendentals=2 * 10**6
        ),
        name="attention",
    )(
        states,
        begins.astype(jnp.int32)[:, None],
        cosine,
        sine,
        attn_gain.reshape(tps, 1, wide),
        mlp_gain.reshape(seqs, 1, depth),
        query_weight,
        key_weight,
        value_weight,
        output_weight,
        gate_weight,
        up_weight,
    )
    return pl.pallas_call(
        down_kernel,
        out_shape=jax.ShapeDtypeStruct((tok, wide), BF16),
        in_specs=[VM, VM, ANY],
        out_specs=VM,
        scratch_shapes=[
            pltpu.VMEM((tps, down.shape[0], wide), BF16),
            *sum_scratch(tps, tok, wide),
            *dma(8, 8, 8),
        ],
        compiler_params=pltpu.CompilerParams(
            collective_id=1, has_side_effects=True, vmem_limit_bytes=60 * 1024 * 1024
        ),
        cost_estimate=pl.CostEstimate(flops=10**10, bytes_accessed=10**7, transcendentals=0),
        name="down",
    )(hidden, mixed, down)


def solution(mesh):
    in_specs = (
        P("seq", "tp"),
        P(),
        P(),
        P(None, "tp"),
        P(None, "tp"),
        P(None, "tp"),
        P("tp", None),
        P(),
        P("seq", "tp"),
        P("seq", "tp"),
        P("tp", "seq"),
    )
    return jax.shard_map(
        per_device, mesh=mesh, in_specs=in_specs, out_specs=P("seq", "tp"), check_vma=False
    )
```

```python
import jax
import jax.numpy as jnp
import numpy as np
from jax import lax
from jax.experimental import pallas as pl
from jax.experimental.pallas import tpu as pltpu
from jax.sharding import PartitionSpec as P

HD = 128
EPS = 1e-05
THETA = 500000.0
MESH = pl.DeviceIdType.MESH
F32 = jnp.float32
BF16 = jnp.bfloat16
VM = pl.BlockSpec(memory_space=pltpu.VMEM)
ANY = pl.BlockSpec(memory_space=pl.ANY)


class Tp:
    def __init__(self):
        me = lax.axis_index("tp")
        y, z = me % 4, me // 4
        o = 1 - z
        self.me = me
        self.yp, self.ym, self.y2 = (z * 4 + (y + k) % 4 for k in (1, 3, 2))
        self.zz = o * 4 + y
        self.zyp, self.zym, self.zy2 = (o * 4 + (y + k) % 4 for k in (1, 3, 2))


class Seq:
    def __init__(self):
        me = lax.axis_index("seq")
        x, h, c = me // 4, (me // 2) % 2, me % 2
        g = 1 - h
        self.me = me
        self.xp, self.xm, self.x2 = (((x + k) % 4) * 4 + h * 2 + c for k in (1, 3, 2))
        self.hh = x * 4 + g * 2 + c
        self.hxp, self.hxm, self.hx2 = (((x + k) % 4) * 4 + g * 2 + c for k in (1, 3, 2))
        self.co = x * 4 + h * 2 + (1 - c)


def sender(axis, send, recv):
    def copy(at, src, dst, to):
        made = pltpu.make_async_remote_copy(
            src_ref=src,
            dst_ref=dst,
            send_sem=send.at[at],
            recv_sem=recv.at[at],
            device_id={axis: to},
            device_id_type=MESH,
        )
        made.start()
        return made

    return copy


def greet(tp, seq):
    barrier = pltpu.get_barrier_semaphore()
    near = [("tp", t) for t in (tp.yp, tp.ym, tp.zz)]
    near += [("seq", s) for s in (seq.xp, seq.xm, seq.hh, seq.co)]
    for axis, to in near:
        pl.semaphore_signal(barrier, inc=1, device_id={axis: to}, device_id_type=MESH)
    pl.semaphore_wait(barrier, len(near))


def tp_gather(tp, own, buf, copy, begun, by_z):
    half = own.shape[0] // 2
    lo, hi = pl.ds(0, half), pl.ds(half, half)
    sent = []

    def go(at, src, dst, to):
        sent.append(copy(at, src, dst, to))
        return sent[-1]

    c = go(2, own, buf.at[tp.me], tp.zz)
    a = go(0, own, buf.at[tp.me], tp.yp)
    b = go(1, own, buf.at[tp.me], tp.ym)
    begun()
    a.wait_recv()
    d = go(3, buf.at[tp.ym, lo], buf.at[tp.ym, lo], tp.yp)
    b.wait_recv()
    e = go(4, buf.at[tp.yp, hi], buf.at[tp.yp, hi], tp.ym)
    c.wait_recv()
    f = go(5, buf.at[tp.zz], buf.at[tp.zz], tp.yp)
    g = go(6, buf.at[tp.zz], buf.at[tp.zz], tp.ym)
    if by_z:
        d.wait_recv()
        h = go(7, buf.at[tp.y2, lo], buf.at[tp.y2, lo], tp.zz)
        e.wait_recv()
        i = go(8, buf.at[tp.y2, hi], buf.at[tp.y2, hi], tp.zz)
        f.wait_recv()
        g.wait_recv()
    else:
        f.wait_recv()
        h = go(7, buf.at[tp.zym, lo], buf.at[tp.zym, lo], tp.yp)
        g.wait_recv()
        i = go(8, buf.at[tp.zyp, hi], buf.at[tp.zyp, hi], tp.ym)
        d.wait_recv()
        e.wait_recv()
    h.wait_recv()
    i.wait_recv()
    for one in sent:
        one.wait_send()


def add_to(ref, *others):
    total = ref[...].astype(F32)
    for other in others:
        total = total + other[...].astype(F32)
    ref[...] = total.astype(ref.dtype)


def tp_sum(tp, fill, part, ra, rb, rc, rd, re, copy):
    half = ra.shape[0] // 2
    lo, hi = pl.ds(0, half), pl.ds(half, half)
    fill(tp.zy2)
    a = copy(0, part.at[tp.zy2], ra, tp.zz)
    fill(tp.zyp)
    b = copy(1, part.at[tp.zyp], rc.at[0], tp.yp)
    fill(tp.zym)
    c = copy(2, part.at[tp.zym], rc.at[1], tp.ym)
    fill(tp.y2)
    fill(tp.zz)
    fill(tp.yp)
    fill(tp.ym)
    fill(tp.me)
    a.wait_recv()
    add_to(part.at[tp.y2], ra)
    d = copy(3, part.at[tp.y2, lo], rb.at[0], tp.ym)
    e = copy(4, part.at[tp.y2, hi], rb.at[1], tp.yp)
    b.wait_recv()
    c.wait_recv()
    add_to(part.at[tp.zz], rc.at[0], rc.at[1])
    f = copy(5, part.at[tp.zz], rd, tp.zz)
    d.wait_recv()
    add_to(part.at[tp.ym, lo], rb.at[0])
    g = copy(6, part.at[tp.ym], re.at[0], tp.ym)
    e.wait_recv()
    add_to(part.at[tp.yp, hi], rb.at[1])
    h = copy(7, part.at[tp.yp], re.at[1], tp.yp)
    for one in (f, g, h):
        one.wait_recv()
    total = part[tp.me].astype(F32) + rd[...].astype(F32)
    total = total + re[0].astype(F32) + re[1].astype(F32)
    for one in (a, b, c, d, e, f, g, h):
        one.wait_send()
    return total


class SeqGather:
    def __init__(self, seq, buf, first, rows, copy, copy_in):
        self.seq, self.buf, self.copy, self.copy_in = seq, buf, copy, copy_in
        self.all = pl.ds(first, rows)
        self.lo, self.hi = pl.ds(first, rows // 2), pl.ds(first + rows // 2, rows // 2)
        self.sent, self.inner, self.by = [], [], {}

    def go(self, at, slot, rows, to):
        ref = self.buf.at[slot, rows]
        self.by[at] = self.copy(at, ref, ref, to)
        self.sent.append(self.by[at])

    def share(self, slot, rows):
        ref = self.buf.at[slot, rows]
        self.inner.append(self.copy_in(len(self.inner), ref, ref, self.seq.co))

    def start_x(self):
        q = self.seq
        self.go(0, q.me, self.all, q.xp)
        self.go(1, q.me, self.all, q.xm)
        self.share(q.me, self.all)

    def start_h(self):
        self.go(2, self.seq.me, self.all, self.seq.hh)

    def own_row(self):
        q = self.seq
        self.by[0].wait_recv()
        self.go(3, q.xm, self.lo, q.xp)
        self.share(q.xm, self.all)
        self.by[1].wait_recv()
        self.go(4, q.xp, self.hi, q.xm)
        self.share(q.xp, self.all)

    def other_row(self):
        q = self.seq
        self.by[2].wait_recv()
        self.go(5, q.hh, self.all, q.xp)
        self.go(6, q.hh, self.all, q.xm)
        self.share(q.hh, self.all)

    def far(self):
        q = self.seq
        self.by[5].wait_recv()
        self.go(7, q.hxm, self.lo, q.xp)
        self.share(q.hxm, self.all)
        self.by[6].wait_recv()
        self.go(8, q.hxp, self.hi, q.xm)
        self.share(q.hxp, self.all)
        self.by[3].wait_recv()
        self.share(q.x2, self.lo)
        self.by[4].wait_recv()
        self.share(q.x2, self.hi)

    def last(self):
        q = self.seq
        self.by[7].wait_recv()
        self.share(q.hx2, self.lo)
        self.by[8].wait_recv()
        self.share(q.hx2, self.hi)
        for one in self.inner:
            one.wait_recv()

    def sends_done(self):
        for one in self.sent + self.inner:
            one.wait_send()


def norm_factor(buf):
    blocks, rows, wide = buf.shape

    def add(t, squares):
        block = buf[t].astype(F32)
        return squares + jnp.sum(block * block, axis=-1, keepdims=True)

    squares = lax.fori_loop(0, blocks, add, jnp.zeros((rows, 1), F32))
    return lax.rsqrt(squares / (blocks * wide) + EPS)


def turned(block, cosine, sine):
    return block * cosine + pltpu.roll(block, HD // 2, 1) * sine


def layer_kernel(
    lengths,
    freq,
    states_hbm,
    gain_hbm,
    mlp_gain_hbm,
    wq_hbm,
    wk_hbm,
    wv_hbm,
    wo_hbm,
    gate_hbm,
    up_hbm,
    down_hbm,
    out,
    gain,
    mlp_gain,
    begins,
    cosine,
    sine,
    mixed,
    hidden,
    rows_all,
    wq,
    wk,
    wv,
    wo,
    qacc,
    kvacc,
    kv,
    query,
    scores,
    best,
    totals,
    attended,
    part,
    ra,
    rb,
    rc,
    rd,
    re,
    mixed_all,
    normed_mlp,
    ff,
    ffacc,
    down,
    load,
    s1,
    r1,
    s2,
    r2,
    s3,
    r3,
    s4,
    r4,
    s5,
    r5,
    s6,
    r6,
    s7,
    r7,
    s8,
    r8,
):
    tp, seq = Tp(), Seq()
    tok, wide = states_hbm.shape
    heads = wq.shape[1] // HD
    states = rows_all.at[tp.me]
    units = gate_hbm.shape[1]
    moves = (
        (states_hbm, states),
        (gate_hbm, ff.at[seq.me, :, :units]),
        (up_hbm, ff.at[seq.me, :, units:]),
        (down_hbm, down.at[seq.me]),
        (wq_hbm, wq),
        (wk_hbm, wk),
        (wv_hbm, wv),
        (wo_hbm, wo),
        (gain_hbm, gain),
        (mlp_gain_hbm, mlp_gain),
    )
    loads = [pltpu.make_async_copy(a, b, load.at[i]) for i, (a, b) in enumerate(moves)]
    for one in loads:
        one.start()
    deep = gate_hbm.shape[0] // 2
    pieces = ((ff, 0, deep), (ff, deep, deep), (down, 0, units))
    weights = [
        SeqGather(
            seq,
            *piece,
            sender("seq", s6.at[i], r6.at[i]),
            sender("seq", s7.at[i], r7.at[i]),
        )
        for i, piece in enumerate(pieces)
    ]
    greet(tp, seq)
    loads[0].wait()

    def begun():
        loads[1].wait()
        loads[2].wait()
        weights[0].start_x()
        weights[0].start_h()
        weights[1].start_x()
        spots = lax.broadcasted_iota(jnp.int32, (tok, 1), 0) + seq.me * tok
        end, start = 0, jnp.zeros((tok, 1), jnp.int32)
        for k in range(lengths.shape[0]):
            end = end + lengths[k]
            start += jnp.where(spots >= end, lengths[k], 0)
        begins[...] = start
        angle = (spots - start).astype(F32) * freq[...]
        side = jnp.where(lax.broadcasted_iota(jnp.int32, angle.shape, 1) < HD // 2, -1.0, 1.0)
        cosine[...] = jnp.cos(angle)
        sine[...] = jnp.sin(angle) * side

    tp_gather(tp, states, rows_all, sender("tp", s1, r1), begun, False)
    weights[0].own_row()
    factor = norm_factor(rows_all)
    qacc[...] = jnp.zeros_like(qacc)
    kvacc[...] = jnp.zeros_like(kvacc)
    for one in loads[4:7] + loads[8:]:
        one.wait()

    def project(t, carry):
        normed = (rows_all[t].astype(F32) * factor * gain[t]).astype(BF16)
        at = pl.ds(pl.multiple_of(t * wide, wide), wide)
        qacc[...] += jnp.dot(normed, wq[at, :], preferred_element_type=F32)
        kvacc[:, :HD] += jnp.dot(normed, wk[at, :], preferred_element_type=F32)
        kvacc[:, HD:] += jnp.dot(normed, wv[at, :], preferred_element_type=F32)
        return carry

    lax.fori_loop(0, rows_all.shape[0], project, 0)
    kv[seq.me, :, :HD] = turned(kvacc[:, :HD], cosine[...], sine[...]).astype(BF16)
    kv[seq.me, :, HD:] = kvacc[:, HD:].astype(BF16)
    for h in range(heads):
        block = qacc[:, h * HD : (h + 1) * HD]
        query[h] = turned(block, cosine[...], sine[...]).astype(BF16)
    keys_values = SeqGather(seq, kv, 0, tok, sender("seq", s2, r2), sender("seq", s3, r3))
    keys_values.start_h()
    keys_values.start_x()
    weights[1].start_h()
    keys_values.own_row()
    keys_values.other_row()
    keys_values.far()
    keys_values.last()
    weights[1].own_row()
    weights[0].other_row()
    loads[3].wait()
    weights[2].start_x()
    weights[2].start_h()

    blocks = scores.shape[0]
    slots = kv.shape[0]
    best[...] = jnp.full_like(best, -1e30)
    totals[...] = jnp.zeros_like(totals)

    def score(j, carry):
        keys = kv[(seq.me + slots - j) % slots, :, :HD]
        cols = lax.broadcasted_iota(jnp.int32, (tok, tok), 1) + (seq.me - j) * tok
        lines = lax.broadcasted_iota(jnp.int32, (tok, tok), 0) + seq.me * tok
        allowed = (cols >= begins[...]) & (cols <= lines)
        for h in range(heads):
            found = lax.dot_general(
                query[h], keys, (((1,), (1,)), ((), ())), preferred_element_type=F32
            )
            masked = jnp.where(allowed, found * HD ** (-0.5), -1e30)
            scores[j, h] = masked
            best[h] = jnp.maximum(best[h], masked)
        return carry

    lax.fori_loop(0, blocks, score, 0)
    weights[0].far()
    weights[1].other_row()
    qacc[...] = jnp.zeros_like(qacc)
    highest = [jnp.max(best[h], axis=-1, keepdims=True) for h in range(heads)]
    for h in range(heads):
        best[h] = jnp.broadcast_to(highest[h], (tok, tok))

    def weigh(j, carry):
        values = kv[(seq.me + slots - j) % slots, :, HD:]
        for h in range(heads):
            shares = jnp.exp(scores[j, h] - best[h])
            totals[h] += shares
            qacc[:, h * HD : (h + 1) * HD] += jnp.dot(
                shares.astype(BF16), values, preferred_element_type=F32
            )
        return carry

    lax.fori_loop(0, blocks, weigh, 0)
    for h in range(heads):
        at = slice(h * HD, (h + 1) * HD)
        total = jnp.sum(totals[h], axis=-1, keepdims=True)
        attended[:, at] = (qacc[:, at] / total).astype(BF16)
    loads[7].wait()
    weights[2].own_row()

    def fill(slot):
        at = pl.ds(pl.multiple_of(slot * wide, wide), wide)
        part[slot] = jnp.dot(attended[...], wo[:, at], preferred_element_type=F32).astype(BF16)

    shares = tp_sum(tp, fill, part, ra, rb, rc, rd, re, sender("tp", s4, r4))
    weights[1].far()
    weights[2].other_row()
    own = (states[...].astype(F32) + shares).astype(BF16)
    mixed[...] = own
    mixed_all[tp.me] = own
    tp_gather(tp, mixed, mixed_all, sender("tp", s5, r5), lambda: None, True)
    factor = norm_factor(mixed_all)
    cut = normed_mlp.shape[2]
    for s in range(normed_mlp.shape[0]):
        at = pl.ds(s * cut % wide, cut)
        block = mixed_all[s * cut // wide, :, at].astype(F32)
        normed_mlp[s] = (block * factor * mlp_gain[s]).astype(BF16)
    weights[0].last()
    weights[1].last()
    weights[2].far()
    ffacc[...] = jnp.zeros_like(ffacc)

    def feed(s, carry):
        for at in (pl.ds(0, units), pl.ds(units, units)):
            terms = ffacc[:, at]
            for k in range(4):
                terms += jnp.dot(
                    normed_mlp[s * 4 + k], ff[s * 4 + k, :, at], preferred_element_type=F32
                )
            ffacc[:, at] = terms
        return carry

    lax.fori_loop(0, normed_mlp.shape[0] // 4, feed, 0)
    gate = ffacc[:, :units]
    hidden[...] = (gate / (1.0 + jnp.exp(-gate)) * ffacc[:, units:]).astype(BF16)
    weights[2].last()

    def fill_down(slot):
        for k in range(wide // cut):
            part[slot, :, k * cut : (k + 1) * cut] = jnp.dot(
                hidden[...], down[slot * (wide // cut) + k], preferred_element_type=F32
            ).astype(BF16)

    shares = tp_sum(tp, fill_down, part, ra, rb, rc, rd, re, sender("tp", s8, r8))
    out[...] = (mixed[...].astype(F32) + shares).astype(BF16)
    for one in [keys_values] + weights:
        one.sends_done()


def sum_scratch(tps, tok, wide):
    return [
        pltpu.VMEM((tps, tok, wide), BF16),
        pltpu.VMEM((tok, wide), BF16),
        pltpu.VMEM((2, tok // 2, wide), BF16),
        pltpu.VMEM((2, tok, wide), BF16),
        pltpu.VMEM((tok, wide), BF16),
        pltpu.VMEM((2, tok, wide), BF16),
    ]


def dma(*counts):
    return [pltpu.SemaphoreType.DMA((n,)) for n in counts]


def per_device(
    states,
    doc_lengths,
    attn_gain,
    query_weight,
    key_weight,
    value_weight,
    output_weight,
    mlp_gain,
    gate_weight,
    up_weight,
    down_weight,
):
    tok, wide = states.shape
    tps, seqs = lax.axis_size("tp"), lax.axis_size("seq")
    heads = query_weight.shape[1] // HD
    depth, units = gate_weight.shape
    half = HD // 2
    freq = THETA ** (-2.0 * np.arange(half) / HD)
    freq = jnp.asarray(np.concatenate([freq, freq])[None, :], F32)
    blocks = min(seqs, 2048 // tok + 1)

    return pl.pallas_call(
        layer_kernel,
        out_shape=jax.ShapeDtypeStruct((tok, wide), BF16),
        in_specs=[pl.BlockSpec(memory_space=pltpu.SMEM), VM] + [ANY] * 10,
        out_specs=VM,
        scratch_shapes=[
            pltpu.VMEM((tps, 1, wide), F32),
            pltpu.VMEM((seqs, 1, depth), F32),
            pltpu.VMEM((tok, 1), jnp.int32),
            pltpu.VMEM((tok, HD), F32),
            pltpu.VMEM((tok, HD), F32),
            pltpu.VMEM((tok, wide), BF16),
            pltpu.VMEM((tok, units), BF16),
            pltpu.VMEM((tps, tok, wide), BF16),
            pltpu.VMEM(query_weight.shape, BF16),
            pltpu.VMEM(key_weight.shape, BF16),
            pltpu.VMEM(value_weight.shape, BF16),
            pltpu.VMEM(output_weight.shape, BF16),
            pltpu.VMEM((tok, heads * HD), F32),
            pltpu.VMEM((tok, 2 * HD), F32),
            pltpu.VMEM((seqs, tok, 2 * HD), BF16),
            pltpu.VMEM((heads, tok, HD), BF16),
            pltpu.VMEM((blocks, heads, tok, tok), F32),
            pltpu.VMEM((heads, tok, tok), F32),
            pltpu.VMEM((heads, tok, tok), F32),
            pltpu.VMEM((tok, heads * HD), BF16),
            *sum_scratch(tps, tok, wide),
            pltpu.VMEM((tps, tok, wide), BF16),
            pltpu.VMEM((seqs, tok, depth), BF16),
            pltpu.VMEM((seqs, depth, 2 * units), BF16),
            pltpu.VMEM((tok, 2 * units), F32),
            pltpu.VMEM((seqs, units, depth), BF16),
            *dma(10, 9, 9, 9, 9, 10, 10, 8, 8, 9, 9),
            *[pltpu.SemaphoreType.DMA((3, n)) for n in (9, 9, 10, 10)],
            *dma(8, 8),
        ],
        compiler_params=pltpu.CompilerParams(
            collective_id=0, has_side_effects=True, vmem_limit_bytes=67043328
        ),
        cost_estimate=pl.CostEstimate(
            flops=6 * 10**10, bytes_accessed=2 * 10**7, transcendentals=2 * 10**6
        ),
        name="layer",
    )(
        doc_lengths,
        freq,
        states,
        attn_gain.reshape(tps, 1, wide),
        mlp_gain.reshape(seqs, 1, depth),
        query_weight,
        key_weight,
        value_weight,
        output_weight,
        gate_weight,
        up_weight,
        down_weight,
    )


def solution(mesh):
    in_specs = (
        P("seq", "tp"),
        P(),
        P(),
        P(None, "tp"),
        P(None, "tp"),
        P(None, "tp"),
        P("tp", None),
        P(),
        P("seq", "tp"),
        P("seq", "tp"),
        P("tp", "seq"),
    )
    return jax.shard_map(
        per_device, mesh=mesh, in_specs=in_specs, out_specs=P("seq", "tp"), check_vma=False
    )
```

```python
import jax
import jax.numpy as jnp
import numpy as np
from jax import lax
from jax.experimental import pallas as pl
from jax.experimental.pallas import tpu as pltpu
from jax.sharding import PartitionSpec as P

HD = 128
EPS = 1e-05
THETA = 500000.0
MESH = pl.DeviceIdType.MESH
F32 = jnp.float32
BF16 = jnp.bfloat16
VM = pl.BlockSpec(memory_space=pltpu.VMEM)
ANY = pl.BlockSpec(memory_space=pl.ANY)


class Tp:
    def __init__(self):
        me = lax.axis_index("tp")
        y, z = me % 4, me // 4
        o = 1 - z
        self.me = me
        self.yp, self.ym, self.y2 = (z * 4 + (y + k) % 4 for k in (1, 3, 2))
        self.zz = o * 4 + y
        self.zyp, self.zym, self.zy2 = (o * 4 + (y + k) % 4 for k in (1, 3, 2))


class Seq:
    def __init__(self):
        me = lax.axis_index("seq")
        x, h, c = me // 4, (me // 2) % 2, me % 2
        g = 1 - h
        self.me = me
        self.xp, self.xm, self.x2 = (((x + k) % 4) * 4 + h * 2 + c for k in (1, 3, 2))
        self.hh = x * 4 + g * 2 + c
        self.hxp, self.hxm, self.hx2 = (((x + k) % 4) * 4 + g * 2 + c for k in (1, 3, 2))
        self.co = x * 4 + h * 2 + (1 - c)


def sender(axis, send, recv):
    def copy(at, src, dst, to):
        made = pltpu.make_async_remote_copy(
            src_ref=src,
            dst_ref=dst,
            send_sem=send.at[at],
            recv_sem=recv.at[at],
            device_id={axis: to},
            device_id_type=MESH,
        )
        made.start()
        return made

    return copy


def greet(tp, seq):
    barrier = pltpu.get_barrier_semaphore()
    near = [("tp", t) for t in (tp.yp, tp.ym, tp.zz)]
    near += [("seq", s) for s in (seq.xp, seq.xm, seq.hh, seq.co)]
    for axis, to in near:
        pl.semaphore_signal(barrier, inc=1, device_id={axis: to}, device_id_type=MESH)
    pl.semaphore_wait(barrier, len(near))


def idle():
    return None


def tp_gather(tp, own, buf, copy, begun, late, by_z):
    half = own.shape[0] // 2
    lo, hi = pl.ds(0, half), pl.ds(half, half)
    sent = []

    def go(at, src, dst, to):
        sent.append(copy(at, src, dst, to))
        return sent[-1]

    c = go(2, own, buf.at[tp.me], tp.zz)
    a = go(0, own, buf.at[tp.me], tp.yp)
    b = go(1, own, buf.at[tp.me], tp.ym)
    begun()
    a.wait_recv()
    d = go(3, buf.at[tp.ym, lo], buf.at[tp.ym, lo], tp.yp)
    b.wait_recv()
    e = go(4, buf.at[tp.yp, hi], buf.at[tp.yp, hi], tp.ym)
    c.wait_recv()
    f = go(5, buf.at[tp.zz], buf.at[tp.zz], tp.yp)
    g = go(6, buf.at[tp.zz], buf.at[tp.zz], tp.ym)
    if by_z:
        d.wait_recv()
        h = go(7, buf.at[tp.y2, lo], buf.at[tp.y2, lo], tp.zz)
        e.wait_recv()
        i = go(8, buf.at[tp.y2, hi], buf.at[tp.y2, hi], tp.zz)
        f.wait_recv()
        g.wait_recv()
    else:
        f.wait_recv()
        h = go(7, buf.at[tp.zym, lo], buf.at[tp.zym, lo], tp.yp)
        g.wait_recv()
        i = go(8, buf.at[tp.zyp, hi], buf.at[tp.zyp, hi], tp.ym)
        d.wait_recv()
        e.wait_recv()
    late()
    h.wait_recv()
    i.wait_recv()
    for one in sent:
        one.wait_send()


def add_to(ref, *others):
    total = ref[...].astype(F32)
    for other in others:
        total = total + other[...].astype(F32)
    ref[...] = total.astype(ref.dtype)


def tp_sum(tp, fill, part, ra, rb, rc, rd, re, copy, begun):
    half = ra.shape[0] // 2
    lo, hi = pl.ds(0, half), pl.ds(half, half)
    fill(tp.zy2)
    a = copy(0, part.at[tp.zy2], ra, tp.zz)
    fill(tp.zyp)
    b = copy(1, part.at[tp.zyp], rc.at[0], tp.yp)
    fill(tp.zym)
    c = copy(2, part.at[tp.zym], rc.at[1], tp.ym)
    fill(tp.y2)
    fill(tp.zz)
    fill(tp.yp)
    fill(tp.ym)
    fill(tp.me)
    a.wait_recv()
    add_to(part.at[tp.y2], ra)
    d = copy(3, part.at[tp.y2, lo], rb.at[0], tp.ym)
    e = copy(4, part.at[tp.y2, hi], rb.at[1], tp.yp)
    b.wait_recv()
    c.wait_recv()
    add_to(part.at[tp.zz], rc.at[0], rc.at[1])
    f = copy(5, part.at[tp.zz], rd, tp.zz)
    begun()
    d.wait_recv()
    add_to(part.at[tp.ym, lo], rb.at[0])
    g = copy(6, part.at[tp.ym], re.at[0], tp.ym)
    e.wait_recv()
    add_to(part.at[tp.yp, hi], rb.at[1])
    h = copy(7, part.at[tp.yp], re.at[1], tp.yp)
    for one in (f, g, h):
        one.wait_recv()
    total = part[tp.me].astype(F32) + rd[...].astype(F32)
    total = total + re[0].astype(F32) + re[1].astype(F32)
    for one in (a, b, c, d, e, f, g, h):
        one.wait_send()
    return total


class SeqGather:
    def __init__(self, seq, buf, first, rows, copy, copy_in):
        self.seq, self.buf, self.copy, self.copy_in = seq, buf, copy, copy_in
        self.all = pl.ds(first, rows)
        self.lo, self.hi = pl.ds(first, rows // 2), pl.ds(first + rows // 2, rows // 2)
        self.sent, self.inner, self.by = [], [], {}

    def go(self, at, slot, rows, to):
        ref = self.buf.at[slot, rows]
        self.by[at] = self.copy(at, ref, ref, to)
        self.sent.append(self.by[at])

    def share(self, slot, rows):
        ref = self.buf.at[slot, rows]
        self.inner.append(self.copy_in(len(self.inner), ref, ref, self.seq.co))

    def start_x(self):
        q = self.seq
        self.go(0, q.me, self.all, q.xp)
        self.go(1, q.me, self.all, q.xm)
        self.share(q.me, self.all)

    def start_h(self):
        self.go(2, self.seq.me, self.all, self.seq.hh)

    def own_row(self):
        q = self.seq
        self.by[0].wait_recv()
        self.go(3, q.xm, self.lo, q.xp)
        self.share(q.xm, self.all)
        self.by[1].wait_recv()
        self.go(4, q.xp, self.hi, q.xm)
        self.share(q.xp, self.all)

    def other_row(self):
        q = self.seq
        self.by[2].wait_recv()
        self.go(5, q.hh, self.all, q.xp)
        self.go(6, q.hh, self.all, q.xm)
        self.share(q.hh, self.all)

    def across(self):
        q = self.seq
        self.by[3].wait_recv()
        self.go(7, q.x2, self.lo, q.hh)
        self.share(q.x2, self.lo)
        self.by[4].wait_recv()
        self.go(8, q.x2, self.hi, q.hh)
        self.share(q.x2, self.hi)

    def far(self):
        q = self.seq
        self.by[5].wait_recv()
        self.share(q.hxm, self.all)
        self.by[6].wait_recv()
        self.share(q.hxp, self.all)

    def end(self):
        q = self.seq
        self.by[7].wait_recv()
        self.share(q.hx2, self.lo)
        self.by[8].wait_recv()
        self.share(q.hx2, self.hi)

    def ready(self):
        for one in self.inner:
            one.wait_recv()

    def sends_done(self):
        for one in self.sent + self.inner:
            one.wait_send()


def norm_factor(buf):
    blocks, rows, wide = buf.shape

    def add(t, squares):
        block = buf[t].astype(F32)
        return squares + jnp.sum(block * block, axis=-1, keepdims=True)

    squares = lax.fori_loop(0, blocks, add, jnp.zeros((rows, 1), F32))
    return lax.rsqrt(squares / (blocks * wide) + EPS)


def turned(block, cosine, sine):
    return block * cosine + pltpu.roll(block, HD // 2, 1) * sine


def layer_kernel(
    lengths,
    freq,
    states_hbm,
    gain_hbm,
    mlp_gain_hbm,
    wq_hbm,
    wk_hbm,
    wv_hbm,
    wo_hbm,
    gate_hbm,
    up_hbm,
    down_hbm,
    out,
    gain,
    mlp_gain,
    begins,
    cosine,
    sine,
    mixed,
    hidden,
    rows_all,
    wq,
    wk,
    wv,
    wo,
    qacc,
    kvacc,
    kv,
    query,
    scores,
    best,
    totals,
    attended,
    part,
    ra,
    rb,
    rc,
    rd,
    re,
    mixed_all,
    normed_mlp,
    gates,
    ups,
    down,
    gate,
    up,
    load,
    s1,
    r1,
    s2,
    r2,
    s3,
    r3,
    s4,
    r4,
    s5,
    r5,
    s6,
    r6,
    s7,
    r7,
    s8,
    r8,
):
    tp, seq = Tp(), Seq()
    tok, wide = states_hbm.shape
    heads = wq.shape[1] // HD
    states = rows_all.at[tp.me]
    units = gate_hbm.shape[1]
    moves = (
        (states_hbm, states),
        (gate_hbm, gates.at[seq.me]),
        (up_hbm, ups.at[seq.me]),
        (down_hbm, down.at[seq.me]),
        (wq_hbm, wq),
        (wk_hbm, wk),
        (wv_hbm, wv),
        (wo_hbm, wo),
        (gain_hbm, gain),
        (mlp_gain_hbm, mlp_gain),
    )
    loads = [pltpu.make_async_copy(a, b, load.at[i]) for i, (a, b) in enumerate(moves)]
    for one in loads:
        one.start()
    pieces = (gates, ups, down)
    weights = [
        SeqGather(
            seq,
            piece,
            0,
            piece.shape[1],
            sender("seq", s6.at[i], r6.at[i]),
            sender("seq", s7.at[i], r7.at[i]),
        )
        for i, piece in enumerate(pieces)
    ]
    greet(tp, seq)
    loads[0].wait()

    def begun():
        loads[1].wait()
        loads[2].wait()
        weights[0].start_x()
        weights[0].start_h()
        weights[1].start_x()
        weights[1].start_h()
        spots = lax.broadcasted_iota(jnp.int32, (tok, 1), 0) + seq.me * tok
        end, start = 0, jnp.zeros((tok, 1), jnp.int32)
        for k in range(lengths.shape[0]):
            end = end + lengths[k]
            start += jnp.where(spots >= end, lengths[k], 0)
        begins[...] = start
        angle = (spots - start).astype(F32) * freq[...]
        side = jnp.where(lax.broadcasted_iota(jnp.int32, angle.shape, 1) < HD // 2, -1.0, 1.0)
        cosine[...] = jnp.cos(angle)
        sine[...] = jnp.sin(angle) * side

    tp_gather(tp, states, rows_all, sender("tp", s1, r1), begun, idle, False)
    factor = norm_factor(rows_all)
    qacc[...] = jnp.zeros_like(qacc)
    kvacc[...] = jnp.zeros_like(kvacc)
    for one in loads[4:7] + loads[8:]:
        one.wait()

    def project(t, carry):
        normed = (rows_all[t].astype(F32) * factor * gain[t]).astype(BF16)
        at = pl.ds(pl.multiple_of(t * wide, wide), wide)
        qacc[...] += jnp.dot(normed, wq[at, :], preferred_element_type=F32)
        kvacc[:, :HD] += jnp.dot(normed, wk[at, :], preferred_element_type=F32)
        kvacc[:, HD:] += jnp.dot(normed, wv[at, :], preferred_element_type=F32)
        return carry

    lax.fori_loop(0, rows_all.shape[0], project, 0)
    kv[seq.me, :, :HD] = turned(kvacc[:, :HD], cosine[...], sine[...]).astype(BF16)
    kv[seq.me, :, HD:] = kvacc[:, HD:].astype(BF16)
    for h in range(heads):
        block = qacc[:, h * HD : (h + 1) * HD]
        query[h] = turned(block, cosine[...], sine[...]).astype(BF16)
    keys_values = SeqGather(seq, kv, 0, tok, sender("seq", s2, r2), sender("seq", s3, r3))
    keys_values.start_h()
    keys_values.start_x()
    keys_values.own_row()
    keys_values.other_row()
    weights[0].own_row()
    weights[0].other_row()
    keys_values.across()
    loads[3].wait()
    weights[2].start_h()
    weights[1].own_row()
    keys_values.far()
    keys_values.end()
    keys_values.ready()

    blocks = scores.shape[0]
    slots = kv.shape[0]
    best[...] = jnp.full_like(best, -1e30)
    totals[...] = jnp.zeros_like(totals)

    def score(j, carry):
        keys = kv[(seq.me + slots - j) % slots, :, :HD]
        cols = lax.broadcasted_iota(jnp.int32, (tok, tok), 1) + (seq.me - j) * tok
        lines = lax.broadcasted_iota(jnp.int32, (tok, tok), 0) + seq.me * tok
        allowed = (cols >= begins[...]) & (cols <= lines)
        for h in range(heads):
            found = lax.dot_general(
                query[h], keys, (((1,), (1,)), ((), ())), preferred_element_type=F32
            )
            masked = jnp.where(allowed, found * HD ** (-0.5), -1e30)
            scores[j, h] = masked
            best[h] = jnp.maximum(best[h], masked)
        return carry

    lax.fori_loop(0, blocks, score, 0)
    qacc[...] = jnp.zeros_like(qacc)
    highest = [jnp.max(best[h], axis=-1, keepdims=True) for h in range(heads)]
    for h in range(heads):
        best[h] = jnp.broadcast_to(highest[h], (tok, tok))

    def weigh(j, carry):
        values = kv[(seq.me + slots - j) % slots, :, HD:]
        for h in range(heads):
            shares = jnp.exp(scores[j, h] - best[h])
            totals[h] += shares
            qacc[:, h * HD : (h + 1) * HD] += jnp.dot(
                shares.astype(BF16), values, preferred_element_type=F32
            )
        return carry

    lax.fori_loop(0, blocks, weigh, 0)
    for h in range(heads):
        at = slice(h * HD, (h + 1) * HD)
        total = jnp.sum(totals[h], axis=-1, keepdims=True)
        attended[:, at] = (qacc[:, at] / total).astype(BF16)
    loads[7].wait()
    weights[1].other_row()
    weights[2].start_x()

    def fill(slot):
        at = pl.ds(pl.multiple_of(slot * wide, wide), wide)
        part[slot] = jnp.dot(attended[...], wo[:, at], preferred_element_type=F32).astype(BF16)

    def middle():
        weights[0].across()
        weights[0].far()

    def late():
        weights[2].own_row()
        weights[2].other_row()
        weights[1].far()
        weights[0].end()

    shares = tp_sum(tp, fill, part, ra, rb, rc, rd, re, sender("tp", s4, r4), middle)
    own = (states[...].astype(F32) + shares).astype(BF16)
    mixed[...] = own
    mixed_all[tp.me] = own
    tp_gather(tp, mixed, mixed_all, sender("tp", s5, r5), weights[1].across, late, False)
    factor = norm_factor(mixed_all)
    cut = normed_mlp.shape[2]
    for s in range(normed_mlp.shape[0]):
        at = pl.ds(s * cut % wide, cut)
        block = mixed_all[s * cut // wide, :, at].astype(F32)
        normed_mlp[s] = (block * factor * mlp_gain[s]).astype(BF16)
    weights[1].end()
    weights[2].across()
    for one, blocks_of, total in ((weights[0], gates, gate), (weights[1], ups, up)):
        one.ready()
        total[...] = jnp.zeros_like(total)

        def feed(s, carry):
            terms = total[...]
            for k in range(4):
                terms += jnp.dot(
                    normed_mlp[s * 4 + k], blocks_of[s * 4 + k], preferred_element_type=F32
                )
            total[...] = terms
            return carry

        lax.fori_loop(0, normed_mlp.shape[0] // 4, feed, 0)
    hidden[...] = (gate[...] / (1.0 + jnp.exp(-gate[...])) * up[...]).astype(BF16)
    weights[2].far()
    weights[2].end()
    weights[2].ready()

    def fill_down(slot):
        for k in range(wide // cut):
            part[slot, :, k * cut : (k + 1) * cut] = jnp.dot(
                hidden[...], down[slot * (wide // cut) + k], preferred_element_type=F32
            ).astype(BF16)

    shares = tp_sum(tp, fill_down, part, ra, rb, rc, rd, re, sender("tp", s8, r8), idle)
    out[...] = (mixed[...].astype(F32) + shares).astype(BF16)
    for one in [keys_values] + weights:
        one.sends_done()


def sum_scratch(tps, tok, wide):
    return [
        pltpu.VMEM((tps, tok, wide), BF16),
        pltpu.VMEM((tok, wide), BF16),
        pltpu.VMEM((2, tok // 2, wide), BF16),
        pltpu.VMEM((2, tok, wide), BF16),
        pltpu.VMEM((tok, wide), BF16),
        pltpu.VMEM((2, tok, wide), BF16),
    ]


def dma(*counts):
    return [pltpu.SemaphoreType.DMA((n,)) for n in counts]


def per_device(
    states,
    doc_lengths,
    attn_gain,
    query_weight,
    key_weight,
    value_weight,
    output_weight,
    mlp_gain,
    gate_weight,
    up_weight,
    down_weight,
):
    tok, wide = states.shape
    tps, seqs = lax.axis_size("tp"), lax.axis_size("seq")
    heads = query_weight.shape[1] // HD
    depth, units = gate_weight.shape
    half = HD // 2
    freq = THETA ** (-2.0 * np.arange(half) / HD)
    freq = jnp.asarray(np.concatenate([freq, freq])[None, :], F32)
    blocks = min(seqs, 2048 // tok + 1)

    return pl.pallas_call(
        layer_kernel,
        out_shape=jax.ShapeDtypeStruct((tok, wide), BF16),
        in_specs=[pl.BlockSpec(memory_space=pltpu.SMEM), VM] + [ANY] * 10,
        out_specs=VM,
        scratch_shapes=[
            pltpu.VMEM((tps, 1, wide), F32),
            pltpu.VMEM((seqs, 1, depth), F32),
            pltpu.VMEM((tok, 1), jnp.int32),
            pltpu.VMEM((tok, HD), F32),
            pltpu.VMEM((tok, HD), F32),
            pltpu.VMEM((tok, wide), BF16),
            pltpu.VMEM((tok, units), BF16),
            pltpu.VMEM((tps, tok, wide), BF16),
            pltpu.VMEM(query_weight.shape, BF16),
            pltpu.VMEM(key_weight.shape, BF16),
            pltpu.VMEM(value_weight.shape, BF16),
            pltpu.VMEM(output_weight.shape, BF16),
            pltpu.VMEM((tok, heads * HD), F32),
            pltpu.VMEM((tok, 2 * HD), F32),
            pltpu.VMEM((seqs, tok, 2 * HD), BF16),
            pltpu.VMEM((heads, tok, HD), BF16),
            pltpu.VMEM((blocks, heads, tok, tok), F32),
            pltpu.VMEM((heads, tok, tok), F32),
            pltpu.VMEM((heads, tok, tok), F32),
            pltpu.VMEM((tok, heads * HD), BF16),
            *sum_scratch(tps, tok, wide),
            pltpu.VMEM((tps, tok, wide), BF16),
            pltpu.VMEM((seqs, tok, depth), BF16),
            pltpu.VMEM((seqs, depth, units), BF16),
            pltpu.VMEM((seqs, depth, units), BF16),
            pltpu.VMEM((seqs, units, depth), BF16),
            pltpu.VMEM((tok, units), F32),
            pltpu.VMEM((tok, units), F32),
            *dma(10, 9, 9, 9, 9, 10, 10, 8, 8, 9, 9),
            *[pltpu.SemaphoreType.DMA((3, n)) for n in (9, 9, 10, 10)],
            *dma(8, 8),
        ],
        compiler_params=pltpu.CompilerParams(
            collective_id=0, has_side_effects=True, vmem_limit_bytes=67043328
        ),
        cost_estimate=pl.CostEstimate(
            flops=6 * 10**10, bytes_accessed=2 * 10**7, transcendentals=2 * 10**6
        ),
        name="layer",
    )(
        doc_lengths,
        freq,
        states,
        attn_gain.reshape(tps, 1, wide),
        mlp_gain.reshape(seqs, 1, depth),
        query_weight,
        key_weight,
        value_weight,
        output_weight,
        gate_weight,
        up_weight,
        down_weight,
    )


def solution(mesh):
    in_specs = (
        P("seq", "tp"),
        P(),
        P(),
        P(None, "tp"),
        P(None, "tp"),
        P(None, "tp"),
        P("tp", None),
        P(),
        P("seq", "tp"),
        P("seq", "tp"),
        P("tp", "seq"),
    )
    return jax.shard_map(
        per_device, mesh=mesh, in_specs=in_specs, out_specs=P("seq", "tp"), check_vma=False
    )
```

```python
import jax
import jax.numpy as jnp
import numpy as np
from jax import lax
from jax.experimental import pallas as pl
from jax.experimental.pallas import tpu as pltpu
from jax.sharding import PartitionSpec as P

HD = 128
EPS = 1e-05
THETA = 500000.0
MESH = pl.DeviceIdType.MESH
F32 = jnp.float32
BF16 = jnp.bfloat16
VM = pl.BlockSpec(memory_space=pltpu.VMEM)
ANY = pl.BlockSpec(memory_space=pl.ANY)


class Tp:
    def __init__(self):
        me = lax.axis_index("tp")
        y, z = me % 4, me // 4
        o = 1 - z
        self.me = me
        self.yp, self.ym, self.y2 = (z * 4 + (y + k) % 4 for k in (1, 3, 2))
        self.zz = o * 4 + y
        self.zyp, self.zym, self.zy2 = (o * 4 + (y + k) % 4 for k in (1, 3, 2))


class Seq:
    def __init__(self):
        me = lax.axis_index("seq")
        x, h, c = me // 4, (me // 2) % 2, me % 2
        g = 1 - h
        self.me = me
        self.xp, self.xm, self.x2 = (((x + k) % 4) * 4 + h * 2 + c for k in (1, 3, 2))
        self.hh = x * 4 + g * 2 + c
        self.hxp, self.hxm, self.hx2 = (((x + k) % 4) * 4 + g * 2 + c for k in (1, 3, 2))
        self.co = x * 4 + h * 2 + (1 - c)


def sender(axis, send, recv):
    def copy(at, src, dst, to):
        made = pltpu.make_async_remote_copy(
            src_ref=src,
            dst_ref=dst,
            send_sem=send.at[at],
            recv_sem=recv.at[at],
            device_id={axis: to},
            device_id_type=MESH,
        )
        made.start()
        return made

    return copy


def greet(tp, seq):
    barrier = pltpu.get_barrier_semaphore()
    near = [("tp", t) for t in (tp.yp, tp.ym, tp.zz)]
    near += [("seq", s) for s in (seq.xp, seq.xm, seq.hh, seq.co)]
    for axis, to in near:
        pl.semaphore_signal(barrier, inc=1, device_id={axis: to}, device_id_type=MESH)
    pl.semaphore_wait(barrier, len(near))


def idle():
    return None


def streams(rows):
    wide = rows // 2
    return [
        (pl.ds(k, wide), pl.ds(k, wide // 2), pl.ds(k + wide // 2, wide // 2))
        for k in (0, wide)
    ]


def tp_gather(tp, own, buf, copy, begun, middle, late, by_z):
    cuts = streams(own.shape[0])
    made = {}

    def go(k, at, src, dst, to):
        made[k, at] = copy(9 * k + at, src, dst, to)

    def pass_on(k, at, slot, rows, to):
        go(k, at, buf.at[slot, rows], buf.at[slot, rows], to)

    for k, (rows, lo, hi) in enumerate(cuts):
        go(k, 2, own.at[rows], buf.at[tp.me, rows], tp.zz)
        go(k, 0, own.at[rows], buf.at[tp.me, rows], tp.yp)
        go(k, 1, own.at[rows], buf.at[tp.me, rows], tp.ym)
    begun()
    for k, (rows, lo, hi) in enumerate(cuts):
        made[k, 0].wait_recv()
        pass_on(k, 3, tp.ym, lo, tp.yp)
        made[k, 1].wait_recv()
        pass_on(k, 4, tp.yp, hi, tp.ym)
        made[k, 2].wait_recv()
        pass_on(k, 5, tp.zz, rows, tp.yp)
        pass_on(k, 6, tp.zz, rows, tp.ym)
    middle()
    for k, (rows, lo, hi) in enumerate(cuts):
        if by_z:
            made[k, 3].wait_recv()
            pass_on(k, 7, tp.y2, lo, tp.zz)
            made[k, 4].wait_recv()
            pass_on(k, 8, tp.y2, hi, tp.zz)
        else:
            made[k, 5].wait_recv()
            pass_on(k, 7, tp.zym, lo, tp.yp)
            made[k, 6].wait_recv()
            pass_on(k, 8, tp.zyp, hi, tp.ym)
    late()
    for k in range(len(cuts)):
        for at in ((5, 6) if by_z else (3, 4)) + (7, 8):
            made[k, at].wait_recv()
    for one in made.values():
        one.wait_send()


def add_to(ref, *others):
    total = ref[...].astype(F32)
    for other in others:
        total = total + other[...].astype(F32)
    ref[...] = total.astype(ref.dtype)


def tp_sum(tp, fill, part, ra, rb, rc, rd, re, copy, begun):
    cuts = streams(ra.shape[0])
    made = {}

    def go(at, slot, to, dst, k, rows):
        made[k, at] = copy(8 * k + at, part.at[slot, rows], dst, to)

    fill(tp.zy2)
    for k, (rows, lo, hi) in enumerate(cuts):
        go(0, tp.zy2, tp.zz, ra.at[rows], k, rows)
    fill(tp.zyp)
    for k, (rows, lo, hi) in enumerate(cuts):
        go(1, tp.zyp, tp.yp, rc.at[0, rows], k, rows)
    fill(tp.zym)
    for k, (rows, lo, hi) in enumerate(cuts):
        go(2, tp.zym, tp.ym, rc.at[1, rows], k, rows)
    fill(tp.y2)
    fill(tp.zz)
    fill(tp.yp)
    fill(tp.ym)
    fill(tp.me)
    deep = rb.shape[1] // 2
    for k, (rows, lo, hi) in enumerate(cuts):
        inner = pl.ds(k * deep, deep)
        made[k, 0].wait_recv()
        add_to(part.at[tp.y2, rows], ra.at[rows])
        go(3, tp.y2, tp.ym, rb.at[0, inner], k, lo)
        go(4, tp.y2, tp.yp, rb.at[1, inner], k, hi)
        made[k, 1].wait_recv()
        made[k, 2].wait_recv()
        add_to(part.at[tp.zz, rows], rc.at[0, rows], rc.at[1, rows])
        go(5, tp.zz, tp.zz, rd.at[rows], k, rows)
    begun()
    for k, (rows, lo, hi) in enumerate(cuts):
        inner = pl.ds(k * deep, deep)
        made[k, 3].wait_recv()
        add_to(part.at[tp.ym, lo], rb.at[0, inner])
        go(6, tp.ym, tp.ym, re.at[0, rows], k, rows)
        made[k, 4].wait_recv()
        add_to(part.at[tp.yp, hi], rb.at[1, inner])
        go(7, tp.yp, tp.yp, re.at[1, rows], k, rows)
    for k in range(len(cuts)):
        for at in (5, 6, 7):
            made[k, at].wait_recv()
    total = part[tp.me].astype(F32) + rd[...].astype(F32)
    total = total + re[0].astype(F32) + re[1].astype(F32)
    for one in made.values():
        one.wait_send()
    return total


class SeqGather:
    def __init__(self, seq, buf, first, rows, copy, copy_in):
        self.seq, self.buf, self.copy, self.copy_in = seq, buf, copy, copy_in
        self.all = pl.ds(first, rows)
        self.lo, self.hi = pl.ds(first, rows // 2), pl.ds(first + rows // 2, rows // 2)
        self.sent, self.inner, self.by = [], [], {}

    def go(self, at, slot, rows, to):
        ref = self.buf.at[slot, rows]
        self.by[at] = self.copy(at, ref, ref, to)
        self.sent.append(self.by[at])

    def share(self, slot, rows):
        ref = self.buf.at[slot, rows]
        self.inner.append(self.copy_in(len(self.inner), ref, ref, self.seq.co))

    def start_x(self):
        q = self.seq
        self.go(0, q.me, self.all, q.xp)
        self.go(1, q.me, self.all, q.xm)
        self.share(q.me, self.all)

    def start_h(self):
        self.go(2, self.seq.me, self.all, self.seq.hh)

    def own_row(self):
        q = self.seq
        self.by[0].wait_recv()
        self.go(3, q.xm, self.lo, q.xp)
        self.share(q.xm, self.all)
        self.by[1].wait_recv()
        self.go(4, q.xp, self.hi, q.xm)
        self.share(q.xp, self.all)

    def other_row(self):
        q = self.seq
        self.by[2].wait_recv()
        self.go(5, q.hh, self.all, q.xp)
        self.go(6, q.hh, self.all, q.xm)
        self.share(q.hh, self.all)

    def across(self):
        q = self.seq
        self.by[3].wait_recv()
        self.go(7, q.x2, self.lo, q.hh)
        self.share(q.x2, self.lo)
        self.by[4].wait_recv()
        self.go(8, q.x2, self.hi, q.hh)
        self.share(q.x2, self.hi)

    def far(self):
        q = self.seq
        self.by[5].wait_recv()
        self.share(q.hxm, self.all)
        self.by[6].wait_recv()
        self.share(q.hxp, self.all)

    def end(self):
        q = self.seq
        self.by[7].wait_recv()
        self.share(q.hx2, self.lo)
        self.by[8].wait_recv()
        self.share(q.hx2, self.hi)

    def ready(self):
        for one in self.inner:
            one.wait_recv()

    def sends_done(self):
        for one in self.sent + self.inner:
            one.wait_send()


def norm_factor(buf):
    blocks, rows, wide = buf.shape

    def add(t, squares):
        block = buf[t].astype(F32)
        return squares + jnp.sum(block * block, axis=-1, keepdims=True)

    squares = lax.fori_loop(0, blocks, add, jnp.zeros((rows, 1), F32))
    return lax.rsqrt(squares / (blocks * wide) + EPS)


def turned(block, cosine, sine):
    return block * cosine + pltpu.roll(block, HD // 2, 1) * sine


def layer_kernel(
    lengths,
    freq,
    states_hbm,
    gain_hbm,
    mlp_gain_hbm,
    wq_hbm,
    wk_hbm,
    wv_hbm,
    wo_hbm,
    gate_hbm,
    up_hbm,
    down_hbm,
    out,
    gain,
    mlp_gain,
    begins,
    cosine,
    sine,
    mixed,
    hidden,
    rows_all,
    wq,
    wk,
    wv,
    wo,
    qacc,
    kvacc,
    kv,
    query,
    scores,
    best,
    totals,
    attended,
    part,
    ra,
    rb,
    rc,
    rd,
    re,
    mixed_all,
    normed_mlp,
    gates,
    ups,
    down,
    gate,
    up,
    load,
    s1,
    r1,
    s2,
    r2,
    s3,
    r3,
    s4,
    r4,
    s5,
    r5,
    s6,
    r6,
    s7,
    r7,
    s8,
    r8,
):
    tp, seq = Tp(), Seq()
    tok, wide = states_hbm.shape
    heads = wq.shape[1] // HD
    states = rows_all.at[tp.me]
    units = gate_hbm.shape[1]
    moves = (
        (states_hbm, states),
        (gate_hbm, gates.at[seq.me]),
        (up_hbm, ups.at[seq.me]),
        (down_hbm, down.at[seq.me]),
        (wq_hbm, wq),
        (wk_hbm, wk),
        (wv_hbm, wv),
        (wo_hbm, wo),
        (gain_hbm, gain),
        (mlp_gain_hbm, mlp_gain),
    )
    loads = [pltpu.make_async_copy(a, b, load.at[i]) for i, (a, b) in enumerate(moves)]
    for one in loads:
        one.start()
    pieces = (gates, ups, down)
    weights = [
        SeqGather(
            seq,
            piece,
            0,
            piece.shape[1],
            sender("seq", s6.at[i], r6.at[i]),
            sender("seq", s7.at[i], r7.at[i]),
        )
        for i, piece in enumerate(pieces)
    ]
    greet(tp, seq)
    loads[0].wait()

    def begun():
        loads[1].wait()
        loads[2].wait()
        weights[0].start_x()
        weights[0].start_h()
        weights[1].start_x()
        weights[1].start_h()
        spots = lax.broadcasted_iota(jnp.int32, (tok, 1), 0) + seq.me * tok
        end, start = 0, jnp.zeros((tok, 1), jnp.int32)
        for k in range(lengths.shape[0]):
            end = end + lengths[k]
            start += jnp.where(spots >= end, lengths[k], 0)
        begins[...] = start
        angle = (spots - start).astype(F32) * freq[...]
        side = jnp.where(lax.broadcasted_iota(jnp.int32, angle.shape, 1) < HD // 2, -1.0, 1.0)
        cosine[...] = jnp.cos(angle)
        sine[...] = jnp.sin(angle) * side

    tp_gather(tp, states, rows_all, sender("tp", s1, r1), begun, idle, idle, False)
    factor = norm_factor(rows_all)
    qacc[...] = jnp.zeros_like(qacc)
    kvacc[...] = jnp.zeros_like(kvacc)
    for one in loads[4:7] + loads[8:]:
        one.wait()

    def project(t, carry):
        normed = (rows_all[t].astype(F32) * factor * gain[t]).astype(BF16)
        at = pl.ds(pl.multiple_of(t * wide, wide), wide)
        qacc[...] += jnp.dot(normed, wq[at, :], preferred_element_type=F32)
        kvacc[:, :HD] += jnp.dot(normed, wk[at, :], preferred_element_type=F32)
        kvacc[:, HD:] += jnp.dot(normed, wv[at, :], preferred_element_type=F32)
        return carry

    lax.fori_loop(0, rows_all.shape[0], project, 0)
    kv[seq.me, :, :HD] = turned(kvacc[:, :HD], cosine[...], sine[...]).astype(BF16)
    kv[seq.me, :, HD:] = kvacc[:, HD:].astype(BF16)
    for h in range(heads):
        block = qacc[:, h * HD : (h + 1) * HD]
        query[h] = turned(block, cosine[...], sine[...]).astype(BF16)
    keys_values = SeqGather(seq, kv, 0, tok, sender("seq", s2, r2), sender("seq", s3, r3))
    keys_values.start_h()
    keys_values.start_x()
    keys_values.own_row()
    keys_values.other_row()
    weights[0].own_row()
    weights[0].other_row()
    keys_values.across()
    loads[3].wait()
    weights[2].start_h()
    weights[1].own_row()
    keys_values.far()
    keys_values.end()
    keys_values.ready()

    blocks = scores.shape[0]
    slots = kv.shape[0]
    best[...] = jnp.full_like(best, -1e30)
    totals[...] = jnp.zeros_like(totals)

    def score(j, carry):
        keys = kv[(seq.me + slots - j) % slots, :, :HD]
        cols = lax.broadcasted_iota(jnp.int32, (tok, tok), 1) + (seq.me - j) * tok
        lines = lax.broadcasted_iota(jnp.int32, (tok, tok), 0) + seq.me * tok
        allowed = (cols >= begins[...]) & (cols <= lines)
        for h in range(heads):
            found = lax.dot_general(
                query[h], keys, (((1,), (1,)), ((), ())), preferred_element_type=F32
            )
            masked = jnp.where(allowed, found * HD ** (-0.5), -1e30)
            scores[j, h] = masked
            best[h] = jnp.maximum(best[h], masked)
        return carry

    lax.fori_loop(0, blocks, score, 0)
    qacc[...] = jnp.zeros_like(qacc)
    highest = [jnp.max(best[h], axis=-1, keepdims=True) for h in range(heads)]
    for h in range(heads):
        best[h] = jnp.broadcast_to(highest[h], (tok, tok))

    def weigh(j, carry):
        values = kv[(seq.me + slots - j) % slots, :, HD:]
        for h in range(heads):
            shares = jnp.exp(scores[j, h] - best[h])
            totals[h] += shares
            qacc[:, h * HD : (h + 1) * HD] += jnp.dot(
                shares.astype(BF16), values, preferred_element_type=F32
            )
        return carry

    lax.fori_loop(0, blocks, weigh, 0)
    for h in range(heads):
        at = slice(h * HD, (h + 1) * HD)
        total = jnp.sum(totals[h], axis=-1, keepdims=True)
        attended[:, at] = (qacc[:, at] / total).astype(BF16)
    loads[7].wait()
    weights[1].other_row()
    weights[2].start_x()

    def fill(slot):
        at = pl.ds(pl.multiple_of(slot * wide, wide), wide)
        part[slot] = jnp.dot(attended[...], wo[:, at], preferred_element_type=F32).astype(BF16)

    def middle():
        weights[0].across()
        weights[0].far()

    def later():
        weights[2].own_row()
        weights[2].other_row()

    def late():
        weights[0].end()
        weights[2].across()
        weights[1].far()

    shares = tp_sum(tp, fill, part, ra, rb, rc, rd, re, sender("tp", s4, r4), middle)
    own = (states[...].astype(F32) + shares).astype(BF16)
    mixed[...] = own
    mixed_all[tp.me] = own
    tp_gather(tp, mixed, mixed_all, sender("tp", s5, r5), weights[1].across, later, late, False)
    factor = norm_factor(mixed_all)
    cut = normed_mlp.shape[2]
    for s in range(normed_mlp.shape[0]):
        at = pl.ds(s * cut % wide, cut)
        block = mixed_all[s * cut // wide, :, at].astype(F32)
        normed_mlp[s] = (block * factor * mlp_gain[s]).astype(BF16)
    weights[1].end()
    for one, blocks_of, total in ((weights[0], gates, gate), (weights[1], ups, up)):
        one.ready()
        total[...] = jnp.zeros_like(total)

        def feed(s, carry):
            terms = total[...]
            for k in range(4):
                terms += jnp.dot(
                    normed_mlp[s * 4 + k], blocks_of[s * 4 + k], preferred_element_type=F32
                )
            total[...] = terms
            return carry

        lax.fori_loop(0, normed_mlp.shape[0] // 4, feed, 0)
    hidden[...] = (gate[...] / (1.0 + jnp.exp(-gate[...])) * up[...]).astype(BF16)
    weights[2].far()
    weights[2].end()
    weights[2].ready()

    def fill_down(slot):
        for k in range(wide // cut):
            part[slot, :, k * cut : (k + 1) * cut] = jnp.dot(
                hidden[...], down[slot * (wide // cut) + k], preferred_element_type=F32
            ).astype(BF16)

    shares = tp_sum(tp, fill_down, part, ra, rb, rc, rd, re, sender("tp", s8, r8), idle)
    out[...] = (mixed[...].astype(F32) + shares).astype(BF16)
    for one in [keys_values] + weights:
        one.sends_done()


def sum_scratch(tps, tok, wide):
    return [
        pltpu.VMEM((tps, tok, wide), BF16),
        pltpu.VMEM((tok, wide), BF16),
        pltpu.VMEM((2, tok // 2, wide), BF16),
        pltpu.VMEM((2, tok, wide), BF16),
        pltpu.VMEM((tok, wide), BF16),
        pltpu.VMEM((2, tok, wide), BF16),
    ]


def dma(*counts):
    return [pltpu.SemaphoreType.DMA((n,)) for n in counts]


def per_device(
    states,
    doc_lengths,
    attn_gain,
    query_weight,
    key_weight,
    value_weight,
    output_weight,
    mlp_gain,
    gate_weight,
    up_weight,
    down_weight,
):
    tok, wide = states.shape
    tps, seqs = lax.axis_size("tp"), lax.axis_size("seq")
    heads = query_weight.shape[1] // HD
    depth, units = gate_weight.shape
    half = HD // 2
    freq = THETA ** (-2.0 * np.arange(half) / HD)
    freq = jnp.asarray(np.concatenate([freq, freq])[None, :], F32)
    blocks = min(seqs, 2048 // tok + 1)

    return pl.pallas_call(
        layer_kernel,
        out_shape=jax.ShapeDtypeStruct((tok, wide), BF16),
        in_specs=[pl.BlockSpec(memory_space=pltpu.SMEM), VM] + [ANY] * 10,
        out_specs=VM,
        scratch_shapes=[
            pltpu.VMEM((tps, 1, wide), F32),
            pltpu.VMEM((seqs, 1, depth), F32),
            pltpu.VMEM((tok, 1), jnp.int32),
            pltpu.VMEM((tok, HD), F32),
            pltpu.VMEM((tok, HD), F32),
            pltpu.VMEM((tok, wide), BF16),
            pltpu.VMEM((tok, units), BF16),
            pltpu.VMEM((tps, tok, wide), BF16),
            pltpu.VMEM(query_weight.shape, BF16),
            pltpu.VMEM(key_weight.shape, BF16),
            pltpu.VMEM(value_weight.shape, BF16),
            pltpu.VMEM(output_weight.shape, BF16),
            pltpu.VMEM((tok, heads * HD), F32),
            pltpu.VMEM((tok, 2 * HD), F32),
            pltpu.VMEM((seqs, tok, 2 * HD), BF16),
            pltpu.VMEM((heads, tok, HD), BF16),
            pltpu.VMEM((blocks, heads, tok, tok), F32),
            pltpu.VMEM((heads, tok, tok), F32),
            pltpu.VMEM((heads, tok, tok), F32),
            pltpu.VMEM((tok, heads * HD), BF16),
            *sum_scratch(tps, tok, wide),
            pltpu.VMEM((tps, tok, wide), BF16),
            pltpu.VMEM((seqs, tok, depth), BF16),
            pltpu.VMEM((seqs, depth, units), BF16),
            pltpu.VMEM((seqs, depth, units), BF16),
            pltpu.VMEM((seqs, units, depth), BF16),
            pltpu.VMEM((tok, units), F32),
            pltpu.VMEM((tok, units), F32),
            *dma(10, 18, 18, 9, 9, 10, 10, 16, 16, 18, 18),
            *[pltpu.SemaphoreType.DMA((3, n)) for n in (9, 9, 10, 10)],
            *dma(16, 16),
        ],
        compiler_params=pltpu.CompilerParams(
            collective_id=0, has_side_effects=True, vmem_limit_bytes=67043328
        ),
        cost_estimate=pl.CostEstimate(
            flops=6 * 10**10, bytes_accessed=2 * 10**7, transcendentals=2 * 10**6
        ),
        name="layer",
    )(
        doc_lengths,
        freq,
        states,
        attn_gain.reshape(tps, 1, wide),
        mlp_gain.reshape(seqs, 1, depth),
        query_weight,
        key_weight,
        value_weight,
        output_weight,
        gate_weight,
        up_weight,
        down_weight,
    )


def solution(mesh):
    in_specs = (
        P("seq", "tp"),
        P(),
        P(),
        P(None, "tp"),
        P(None, "tp"),
        P(None, "tp"),
        P("tp", None),
        P(),
        P("seq", "tp"),
        P("seq", "tp"),
        P("tp", "seq"),
    )
    return jax.shard_map(
        per_device, mesh=mesh, in_specs=in_specs, out_specs=P("seq", "tp"), check_vma=False
    )
```

```python
import jax
import jax.numpy as jnp
import numpy as np
from jax import lax
from jax.experimental import pallas as pl
from jax.experimental.pallas import tpu as pltpu
from jax.sharding import PartitionSpec as P

HD = 128
EPS = 1e-05
THETA = 500000.0
MESH = pl.DeviceIdType.MESH
F32 = jnp.float32
BF16 = jnp.bfloat16
VM = pl.BlockSpec(memory_space=pltpu.VMEM)
ANY = pl.BlockSpec(memory_space=pl.ANY)


class Tp:
    def __init__(self):
        me = lax.axis_index("tp")
        y, z = me % 4, me // 4
        o = 1 - z
        self.me = me
        self.yp, self.ym, self.y2 = (z * 4 + (y + k) % 4 for k in (1, 3, 2))
        self.zz = o * 4 + y
        self.zyp, self.zym, self.zy2 = (o * 4 + (y + k) % 4 for k in (1, 3, 2))


class Seq:
    def __init__(self):
        me = lax.axis_index("seq")
        x, h, c = me // 4, (me // 2) % 2, me % 2
        g = 1 - h
        self.me = me
        self.xp, self.xm, self.x2 = (((x + k) % 4) * 4 + h * 2 + c for k in (1, 3, 2))
        self.hh = x * 4 + g * 2 + c
        self.hxp, self.hxm, self.hx2 = (((x + k) % 4) * 4 + g * 2 + c for k in (1, 3, 2))
        self.co = x * 4 + h * 2 + (1 - c)


def sender(axis, send, recv):
    def copy(at, src, dst, to):
        made = pltpu.make_async_remote_copy(
            src_ref=src,
            dst_ref=dst,
            send_sem=send.at[at],
            recv_sem=recv.at[at],
            device_id={axis: to},
            device_id_type=MESH,
        )
        made.start()
        return made

    return copy


def greet(tp, seq):
    barrier = pltpu.get_barrier_semaphore()
    near = [("tp", t) for t in (tp.yp, tp.ym, tp.zz)]
    near += [("seq", s) for s in (seq.xp, seq.xm, seq.hh, seq.co)]
    for axis, to in near:
        pl.semaphore_signal(barrier, inc=1, device_id={axis: to}, device_id_type=MESH)
    pl.semaphore_wait(barrier, len(near))


def idle():
    return None


def streams(rows):
    wide = rows // 4
    return [
        (pl.ds(k, wide), pl.ds(k, wide // 2), pl.ds(k + wide // 2, wide // 2))
        for k in range(0, rows, wide)
    ]


def tp_gather(tp, own, buf, copy, begun, middle, late, by_z):
    cuts = streams(own.shape[0])
    made = {}

    def go(k, at, src, dst, to):
        made[k, at] = copy(9 * k + at, src, dst, to)

    def pass_on(k, at, slot, rows, to):
        go(k, at, buf.at[slot, rows], buf.at[slot, rows], to)

    for k, (rows, lo, hi) in enumerate(cuts):
        go(k, 2, own.at[rows], buf.at[tp.me, rows], tp.zz)
        go(k, 0, own.at[rows], buf.at[tp.me, rows], tp.yp)
        go(k, 1, own.at[rows], buf.at[tp.me, rows], tp.ym)
    begun()
    for k, (rows, lo, hi) in enumerate(cuts):
        made[k, 0].wait_recv()
        pass_on(k, 3, tp.ym, lo, tp.yp)
        made[k, 1].wait_recv()
        pass_on(k, 4, tp.yp, hi, tp.ym)
        made[k, 2].wait_recv()
        pass_on(k, 5, tp.zz, rows, tp.yp)
        pass_on(k, 6, tp.zz, rows, tp.ym)
    middle()
    for k, (rows, lo, hi) in enumerate(cuts):
        if by_z:
            made[k, 3].wait_recv()
            pass_on(k, 7, tp.y2, lo, tp.zz)
            made[k, 4].wait_recv()
            pass_on(k, 8, tp.y2, hi, tp.zz)
        else:
            made[k, 5].wait_recv()
            pass_on(k, 7, tp.zym, lo, tp.yp)
            made[k, 6].wait_recv()
            pass_on(k, 8, tp.zyp, hi, tp.ym)
    late()
    for k in range(len(cuts)):
        for at in ((5, 6) if by_z else (3, 4)) + (7, 8):
            made[k, at].wait_recv()
    for one in made.values():
        one.wait_send()


def add_to(ref, *others):
    total = ref[...].astype(F32)
    for other in others:
        total = total + other[...].astype(F32)
    ref[...] = total.astype(ref.dtype)


def tp_sum(tp, fill, part, ra, rb, rc, rd, re, copy, begun):
    cuts = streams(ra.shape[0])
    made = {}

    def go(at, slot, to, dst, k, rows):
        made[k, at] = copy(8 * k + at, part.at[slot, rows], dst, to)

    fill(tp.zy2)
    for k, (rows, lo, hi) in enumerate(cuts):
        go(0, tp.zy2, tp.zz, ra.at[rows], k, rows)
    fill(tp.zyp)
    for k, (rows, lo, hi) in enumerate(cuts):
        go(1, tp.zyp, tp.yp, rc.at[0, rows], k, rows)
    fill(tp.zym)
    for k, (rows, lo, hi) in enumerate(cuts):
        go(2, tp.zym, tp.ym, rc.at[1, rows], k, rows)
    fill(tp.y2)
    fill(tp.zz)
    fill(tp.yp)
    fill(tp.ym)
    fill(tp.me)
    deep = rb.shape[1] // 4
    for k, (rows, lo, hi) in enumerate(cuts):
        inner = pl.ds(k * deep, deep)
        made[k, 0].wait_recv()
        add_to(part.at[tp.y2, rows], ra.at[rows])
        go(3, tp.y2, tp.ym, rb.at[0, inner], k, lo)
        go(4, tp.y2, tp.yp, rb.at[1, inner], k, hi)
        made[k, 1].wait_recv()
        made[k, 2].wait_recv()
        add_to(part.at[tp.zz, rows], rc.at[0, rows], rc.at[1, rows])
        go(5, tp.zz, tp.zz, rd.at[rows], k, rows)
    begun()
    for k, (rows, lo, hi) in enumerate(cuts):
        inner = pl.ds(k * deep, deep)
        made[k, 3].wait_recv()
        add_to(part.at[tp.ym, lo], rb.at[0, inner])
        go(6, tp.ym, tp.ym, re.at[0, rows], k, rows)
        made[k, 4].wait_recv()
        add_to(part.at[tp.yp, hi], rb.at[1, inner])
        go(7, tp.yp, tp.yp, re.at[1, rows], k, rows)
    for k in range(len(cuts)):
        for at in (5, 6, 7):
            made[k, at].wait_recv()
    total = part[tp.me].astype(F32) + rd[...].astype(F32)
    total = total + re[0].astype(F32) + re[1].astype(F32)
    for one in made.values():
        one.wait_send()
    return total


class SeqGather:
    def __init__(self, seq, buf, first, rows, copy, copy_in):
        self.seq, self.buf, self.copy, self.copy_in = seq, buf, copy, copy_in
        self.all = pl.ds(first, rows)
        self.lo, self.hi = pl.ds(first, rows // 2), pl.ds(first + rows // 2, rows // 2)
        self.sent, self.inner, self.by = [], [], {}

    def go(self, at, slot, rows, to):
        ref = self.buf.at[slot, rows]
        self.by[at] = self.copy(at, ref, ref, to)
        self.sent.append(self.by[at])

    def share(self, slot, rows):
        ref = self.buf.at[slot, rows]
        self.inner.append(self.copy_in(len(self.inner), ref, ref, self.seq.co))

    def start_x(self):
        q = self.seq
        self.go(0, q.me, self.all, q.xp)
        self.go(1, q.me, self.all, q.xm)
        self.share(q.me, self.all)

    def start_h(self):
        self.go(2, self.seq.me, self.all, self.seq.hh)

    def own_row(self):
        q = self.seq
        self.by[0].wait_recv()
        self.go(3, q.xm, self.lo, q.xp)
        self.share(q.xm, self.all)
        self.by[1].wait_recv()
        self.go(4, q.xp, self.hi, q.xm)
        self.share(q.xp, self.all)

    def other_row(self):
        q = self.seq
        self.by[2].wait_recv()
        self.go(5, q.hh, self.all, q.xp)
        self.go(6, q.hh, self.all, q.xm)
        self.share(q.hh, self.all)

    def across(self):
        q = self.seq
        self.by[3].wait_recv()
        self.go(7, q.x2, self.lo, q.hh)
        self.share(q.x2, self.lo)
        self.by[4].wait_recv()
        self.go(8, q.x2, self.hi, q.hh)
        self.share(q.x2, self.hi)

    def far(self):
        q = self.seq
        self.by[5].wait_recv()
        self.share(q.hxm, self.all)
        self.by[6].wait_recv()
        self.share(q.hxp, self.all)

    def end(self):
        q = self.seq
        self.by[7].wait_recv()
        self.share(q.hx2, self.lo)
        self.by[8].wait_recv()
        self.share(q.hx2, self.hi)

    def ready(self):
        for one in self.inner:
            one.wait_recv()

    def sends_done(self):
        for one in self.sent + self.inner:
            one.wait_send()


def norm_factor(buf):
    blocks, rows, wide = buf.shape

    def add(t, squares):
        block = buf[t].astype(F32)
        return squares + jnp.sum(block * block, axis=-1, keepdims=True)

    squares = lax.fori_loop(0, blocks, add, jnp.zeros((rows, 1), F32))
    return lax.rsqrt(squares / (blocks * wide) + EPS)


def turned(block, cosine, sine):
    return block * cosine + pltpu.roll(block, HD // 2, 1) * sine


def layer_kernel(
    lengths,
    freq,
    states_hbm,
    gain_hbm,
    mlp_gain_hbm,
    wq_hbm,
    wk_hbm,
    wv_hbm,
    wo_hbm,
    gate_hbm,
    up_hbm,
    down_hbm,
    out,
    gain,
    mlp_gain,
    begins,
    cosine,
    sine,
    mixed,
    hidden,
    rows_all,
    wq,
    wk,
    wv,
    wo,
    qacc,
    kvacc,
    kv,
    query,
    scores,
    best,
    totals,
    attended,
    part,
    ra,
    rb,
    rc,
    rd,
    re,
    mixed_all,
    normed_mlp,
    gates,
    ups,
    down,
    gate,
    up,
    load,
    s1,
    r1,
    s2,
    r2,
    s3,
    r3,
    s4,
    r4,
    s5,
    r5,
    s6,
    r6,
    s7,
    r7,
    s8,
    r8,
):
    tp, seq = Tp(), Seq()
    tok, wide = states_hbm.shape
    heads = wq.shape[1] // HD
    states = rows_all.at[tp.me]
    units = gate_hbm.shape[1]
    moves = (
        (states_hbm, states),
        (gate_hbm, gates.at[seq.me]),
        (up_hbm, ups.at[seq.me]),
        (down_hbm, down.at[seq.me]),
        (wq_hbm, wq),
        (wk_hbm, wk),
        (wv_hbm, wv),
        (wo_hbm, wo),
        (gain_hbm, gain),
        (mlp_gain_hbm, mlp_gain),
    )
    loads = [pltpu.make_async_copy(a, b, load.at[i]) for i, (a, b) in enumerate(moves)]
    for one in loads[:3]:
        one.start()
    pieces = (gates, ups, down)
    weights = [
        SeqGather(
            seq,
            piece,
            0,
            piece.shape[1],
            sender("seq", s6.at[i], r6.at[i]),
            sender("seq", s7.at[i], r7.at[i]),
        )
        for i, piece in enumerate(pieces)
    ]
    greet(tp, seq)
    loads[0].wait()

    def begun():
        loads[1].wait()
        loads[2].wait()
        weights[0].start_x()
        weights[0].start_h()
        weights[1].start_x()
        weights[1].start_h()
        for one in loads[3:]:
            one.start()
        spots = lax.broadcasted_iota(jnp.int32, (tok, 1), 0) + seq.me * tok
        end, start = 0, jnp.zeros((tok, 1), jnp.int32)
        for k in range(lengths.shape[0]):
            end = end + lengths[k]
            start += jnp.where(spots >= end, lengths[k], 0)
        begins[...] = start
        angle = (spots - start).astype(F32) * freq[...]
        side = jnp.where(lax.broadcasted_iota(jnp.int32, angle.shape, 1) < HD // 2, -1.0, 1.0)
        cosine[...] = jnp.cos(angle)
        sine[...] = jnp.sin(angle) * side

    tp_gather(tp, states, rows_all, sender("tp", s1, r1), begun, idle, idle, False)
    factor = norm_factor(rows_all)
    qacc[...] = jnp.zeros_like(qacc)
    kvacc[...] = jnp.zeros_like(kvacc)
    for one in loads[4:7] + loads[8:]:
        one.wait()

    def project(t, carry):
        normed = (rows_all[t].astype(F32) * factor * gain[t]).astype(BF16)
        at = pl.ds(pl.multiple_of(t * wide, wide), wide)
        qacc[...] += jnp.dot(normed, wq[at, :], preferred_element_type=F32)
        kvacc[:, :HD] += jnp.dot(normed, wk[at, :], preferred_element_type=F32)
        kvacc[:, HD:] += jnp.dot(normed, wv[at, :], preferred_element_type=F32)
        return carry

    lax.fori_loop(0, rows_all.shape[0], project, 0)
    kv[seq.me, :, :HD] = turned(kvacc[:, :HD], cosine[...], sine[...]).astype(BF16)
    kv[seq.me, :, HD:] = kvacc[:, HD:].astype(BF16)
    for h in range(heads):
        block = qacc[:, h * HD : (h + 1) * HD]
        query[h] = turned(block, cosine[...], sine[...]).astype(BF16)
    keys_values = SeqGather(seq, kv, 0, tok, sender("seq", s2, r2), sender("seq", s3, r3))
    keys_values.start_h()
    keys_values.start_x()
    keys_values.own_row()
    keys_values.other_row()
    weights[0].own_row()
    weights[0].other_row()
    keys_values.across()
    loads[3].wait()
    weights[2].start_h()
    weights[1].own_row()
    keys_values.far()
    keys_values.end()
    keys_values.ready()

    blocks = scores.shape[0]
    slots = kv.shape[0]
    best[...] = jnp.full_like(best, -1e30)
    totals[...] = jnp.zeros_like(totals)

    def score(j, carry):
        keys = kv[(seq.me + slots - j) % slots, :, :HD]
        cols = lax.broadcasted_iota(jnp.int32, (tok, tok), 1) + (seq.me - j) * tok
        lines = lax.broadcasted_iota(jnp.int32, (tok, tok), 0) + seq.me * tok
        allowed = (cols >= begins[...]) & (cols <= lines)
        for h in range(heads):
            found = lax.dot_general(
                query[h], keys, (((1,), (1,)), ((), ())), preferred_element_type=F32
            )
            masked = jnp.where(allowed, found * HD ** (-0.5), -1e30)
            scores[j, h] = masked
            best[h] = jnp.maximum(best[h], masked)
        return carry

    lax.fori_loop(0, blocks, score, 0)
    qacc[...] = jnp.zeros_like(qacc)
    highest = [jnp.max(best[h], axis=-1, keepdims=True) for h in range(heads)]
    for h in range(heads):
        best[h] = jnp.broadcast_to(highest[h], (tok, tok))

    def weigh(j, carry):
        values = kv[(seq.me + slots - j) % slots, :, HD:]
        for h in range(heads):
            shares = jnp.exp(scores[j, h] - best[h])
            totals[h] += shares
            qacc[:, h * HD : (h + 1) * HD] += jnp.dot(
                shares.astype(BF16), values, preferred_element_type=F32
            )
        return carry

    lax.fori_loop(0, blocks, weigh, 0)
    for h in range(heads):
        at = slice(h * HD, (h + 1) * HD)
        total = jnp.sum(totals[h], axis=-1, keepdims=True)
        attended[:, at] = (qacc[:, at] / total).astype(BF16)
    loads[7].wait()
    weights[2].start_x()
    weights[1].other_row()

    def fill(slot):
        at = pl.ds(pl.multiple_of(slot * wide, wide), wide)
        part[slot] = jnp.dot(attended[...], wo[:, at], preferred_element_type=F32).astype(BF16)

    def middle():
        weights[0].across()
        weights[0].far()

    def early():
        weights[1].across()
        weights[2].own_row()
        weights[2].other_row()

    def late():
        weights[0].end()
        weights[2].across()
        weights[1].far()

    shares = tp_sum(tp, fill, part, ra, rb, rc, rd, re, sender("tp", s4, r4), middle)
    own = (states[...].astype(F32) + shares).astype(BF16)
    mixed[...] = own
    mixed_all[tp.me] = own
    tp_gather(tp, mixed, mixed_all, sender("tp", s5, r5), early, idle, late, False)
    factor = norm_factor(mixed_all)
    cut = normed_mlp.shape[2]
    for s in range(normed_mlp.shape[0]):
        at = pl.ds(s * cut % wide, cut)
        block = mixed_all[s * cut // wide, :, at].astype(F32)
        normed_mlp[s] = (block * factor * mlp_gain[s]).astype(BF16)
    weights[1].end()
    for one, blocks_of, total in ((weights[0], gates, gate), (weights[1], ups, up)):
        one.ready()
        total[...] = jnp.zeros_like(total)

        def feed(s, carry):
            terms = total[...]
            for k in range(4):
                terms += jnp.dot(
                    normed_mlp[s * 4 + k], blocks_of[s * 4 + k], preferred_element_type=F32
                )
            total[...] = terms
            return carry

        lax.fori_loop(0, normed_mlp.shape[0] // 4, feed, 0)
    hidden[...] = (gate[...] / (1.0 + jnp.exp(-gate[...])) * up[...]).astype(BF16)
    weights[2].far()
    weights[2].end()
    weights[2].ready()

    def fill_down(slot):
        for k in range(wide // cut):
            part[slot, :, k * cut : (k + 1) * cut] = jnp.dot(
                hidden[...], down[slot * (wide // cut) + k], preferred_element_type=F32
            ).astype(BF16)

    shares = tp_sum(tp, fill_down, part, ra, rb, rc, rd, re, sender("tp", s8, r8), idle)
    out[...] = (mixed[...].astype(F32) + shares).astype(BF16)
    for one in [keys_values] + weights:
        one.sends_done()


def sum_scratch(tps, tok, wide):
    return [
        pltpu.VMEM((tps, tok, wide), BF16),
        pltpu.VMEM((tok, wide), BF16),
        pltpu.VMEM((2, tok // 2, wide), BF16),
        pltpu.VMEM((2, tok, wide), BF16),
        pltpu.VMEM((tok, wide), BF16),
        pltpu.VMEM((2, tok, wide), BF16),
    ]


def dma(*counts):
    return [pltpu.SemaphoreType.DMA((n,)) for n in counts]


def per_device(
    states,
    doc_lengths,
    attn_gain,
    query_weight,
    key_weight,
    value_weight,
    output_weight,
    mlp_gain,
    gate_weight,
    up_weight,
    down_weight,
):
    tok, wide = states.shape
    tps, seqs = lax.axis_size("tp"), lax.axis_size("seq")
    heads = query_weight.shape[1] // HD
    depth, units = gate_weight.shape
    half = HD // 2
    freq = THETA ** (-2.0 * np.arange(half) / HD)
    freq = jnp.asarray(np.concatenate([freq, freq])[None, :], F32)
    blocks = min(seqs, 2048 // tok + 1)

    return pl.pallas_call(
        layer_kernel,
        out_shape=jax.ShapeDtypeStruct((tok, wide), BF16),
        in_specs=[pl.BlockSpec(memory_space=pltpu.SMEM), VM] + [ANY] * 10,
        out_specs=VM,
        scratch_shapes=[
            pltpu.VMEM((tps, 1, wide), F32),
            pltpu.VMEM((seqs, 1, depth), F32),
            pltpu.VMEM((tok, 1), jnp.int32),
            pltpu.VMEM((tok, HD), F32),
            pltpu.VMEM((tok, HD), F32),
            pltpu.VMEM((tok, wide), BF16),
            pltpu.VMEM((tok, units), BF16),
            pltpu.VMEM((tps, tok, wide), BF16),
            pltpu.VMEM(query_weight.shape, BF16),
            pltpu.VMEM(key_weight.shape, BF16),
            pltpu.VMEM(value_weight.shape, BF16),
            pltpu.VMEM(output_weight.shape, BF16),
            pltpu.VMEM((tok, heads * HD), F32),
            pltpu.VMEM((tok, 2 * HD), F32),
            pltpu.VMEM((seqs, tok, 2 * HD), BF16),
            pltpu.VMEM((heads, tok, HD), BF16),
            pltpu.VMEM((blocks, heads, tok, tok), F32),
            pltpu.VMEM((heads, tok, tok), F32),
            pltpu.VMEM((heads, tok, tok), F32),
            pltpu.VMEM((tok, heads * HD), BF16),
            *sum_scratch(tps, tok, wide),
            pltpu.VMEM((tps, tok, wide), BF16),
            pltpu.VMEM((seqs, tok, depth), BF16),
            pltpu.VMEM((seqs, depth, units), BF16),
            pltpu.VMEM((seqs, depth, units), BF16),
            pltpu.VMEM((seqs, units, depth), BF16),
            pltpu.VMEM((tok, units), F32),
            pltpu.VMEM((tok, units), F32),
            *dma(10, 36, 36, 9, 9, 10, 10, 32, 32, 36, 36),
            *[pltpu.SemaphoreType.DMA((3, n)) for n in (9, 9, 10, 10)],
            *dma(32, 32),
        ],
        compiler_params=pltpu.CompilerParams(
            collective_id=0, has_side_effects=True, vmem_limit_bytes=67043328
        ),
        cost_estimate=pl.CostEstimate(
            flops=6 * 10**10, bytes_accessed=2 * 10**7, transcendentals=2 * 10**6
        ),
        name="layer",
    )(
        doc_lengths,
        freq,
        states,
        attn_gain.reshape(tps, 1, wide),
        mlp_gain.reshape(seqs, 1, depth),
        query_weight,
        key_weight,
        value_weight,
        output_weight,
        gate_weight,
        up_weight,
        down_weight,
    )


def solution(mesh):
    in_specs = (
        P("seq", "tp"),
        P(),
        P(),
        P(None, "tp"),
        P(None, "tp"),
        P(None, "tp"),
        P("tp", None),
        P(),
        P("seq", "tp"),
        P("seq", "tp"),
        P("tp", "seq"),
    )
    return jax.shard_map(
        per_device, mesh=mesh, in_specs=in_specs, out_specs=P("seq", "tp"), check_vma=False
    )
```

```python
import jax
import jax.numpy as jnp
import numpy as np
from jax import lax
from jax.experimental import pallas as pl
from jax.experimental.pallas import tpu as pltpu
from jax.sharding import PartitionSpec as P

HD = 128
EPS = 1e-05
THETA = 500000.0
MESH = pl.DeviceIdType.MESH
F32 = jnp.float32
BF16 = jnp.bfloat16
VM = pl.BlockSpec(memory_space=pltpu.VMEM)
ANY = pl.BlockSpec(memory_space=pl.ANY)


class Tp:
    def __init__(self):
        me = lax.axis_index("tp")
        y, z = me % 4, me // 4
        o = 1 - z
        self.me = me
        self.yp, self.ym, self.y2 = (z * 4 + (y + k) % 4 for k in (1, 3, 2))
        self.zz = o * 4 + y
        self.zyp, self.zym, self.zy2 = (o * 4 + (y + k) % 4 for k in (1, 3, 2))


class Seq:
    def __init__(self):
        me = lax.axis_index("seq")
        x, h, c = me // 4, (me // 2) % 2, me % 2
        g = 1 - h
        self.me = me
        self.xp, self.xm, self.x2 = (((x + k) % 4) * 4 + h * 2 + c for k in (1, 3, 2))
        self.hh = x * 4 + g * 2 + c
        self.hxp, self.hxm, self.hx2 = (((x + k) % 4) * 4 + g * 2 + c for k in (1, 3, 2))
        self.co = x * 4 + h * 2 + (1 - c)


def sender(axis, send, recv):
    def copy(at, src, dst, to):
        made = pltpu.make_async_remote_copy(
            src_ref=src,
            dst_ref=dst,
            send_sem=send.at[at],
            recv_sem=recv.at[at],
            device_id={axis: to},
            device_id_type=MESH,
        )
        made.start()
        return made

    return copy


def greet(tp, seq):
    barrier = pltpu.get_barrier_semaphore()
    near = [("tp", t) for t in (tp.yp, tp.ym, tp.zz)]
    near += [("seq", s) for s in (seq.xp, seq.xm, seq.hh, seq.co)]
    for axis, to in near:
        pl.semaphore_signal(barrier, inc=1, device_id={axis: to}, device_id_type=MESH)
    pl.semaphore_wait(barrier, len(near))


def idle():
    return None


def streams(rows):
    wide = rows // 4
    return [
        (pl.ds(k, wide), pl.ds(k, wide // 2), pl.ds(k + wide // 2, wide // 2))
        for k in range(0, rows, wide)
    ]


def tp_gather(tp, own, buf, copy, begun, middle, late, by_z):
    cuts = streams(own.shape[0])
    made = {}

    def go(k, at, src, dst, to):
        made[k, at] = copy(9 * k + at, src, dst, to)

    def pass_on(k, at, slot, rows, to):
        go(k, at, buf.at[slot, rows], buf.at[slot, rows], to)

    for k, (rows, lo, hi) in enumerate(cuts):
        go(k, 2, own.at[rows], buf.at[tp.me, rows], tp.zz)
        go(k, 0, own.at[rows], buf.at[tp.me, rows], tp.yp)
        go(k, 1, own.at[rows], buf.at[tp.me, rows], tp.ym)
    begun()
    for k, (rows, lo, hi) in enumerate(cuts):
        made[k, 0].wait_recv()
        pass_on(k, 3, tp.ym, lo, tp.yp)
        made[k, 1].wait_recv()
        pass_on(k, 4, tp.yp, hi, tp.ym)
        made[k, 2].wait_recv()
        pass_on(k, 5, tp.zz, rows, tp.yp)
        pass_on(k, 6, tp.zz, rows, tp.ym)
    middle()
    for k, (rows, lo, hi) in enumerate(cuts):
        if by_z:
            made[k, 3].wait_recv()
            pass_on(k, 7, tp.y2, lo, tp.zz)
            made[k, 4].wait_recv()
            pass_on(k, 8, tp.y2, hi, tp.zz)
        else:
            made[k, 5].wait_recv()
            pass_on(k, 7, tp.zym, lo, tp.yp)
            made[k, 6].wait_recv()
            pass_on(k, 8, tp.zyp, hi, tp.ym)
    late()
    for k in range(len(cuts)):
        for at in ((5, 6) if by_z else (3, 4)) + (7, 8):
            made[k, at].wait_recv()
    for one in made.values():
        one.wait_send()


def add_to(ref, *others):
    total = ref[...].astype(F32)
    for other in others:
        total = total + other[...].astype(F32)
    ref[...] = total.astype(ref.dtype)


def tp_sum(tp, fill, part, ra, rb, rc, rd, re, copy, begun):
    cuts = streams(ra.shape[0])
    made = {}

    def go(at, slot, to, dst, k, rows):
        made[k, at] = copy(8 * k + at, part.at[slot, rows], dst, to)

    fill(tp.zy2)
    for k, (rows, lo, hi) in enumerate(cuts):
        go(0, tp.zy2, tp.zz, ra.at[rows], k, rows)
    fill(tp.zyp)
    for k, (rows, lo, hi) in enumerate(cuts):
        go(1, tp.zyp, tp.yp, rc.at[0, rows], k, rows)
    fill(tp.zym)
    for k, (rows, lo, hi) in enumerate(cuts):
        go(2, tp.zym, tp.ym, rc.at[1, rows], k, rows)
    fill(tp.y2)
    fill(tp.zz)
    fill(tp.yp)
    fill(tp.ym)
    fill(tp.me)
    deep = rb.shape[1] // 4
    for k, (rows, lo, hi) in enumerate(cuts):
        inner = pl.ds(k * deep, deep)
        made[k, 0].wait_recv()
        add_to(part.at[tp.y2, rows], ra.at[rows])
        go(3, tp.y2, tp.ym, rb.at[0, inner], k, lo)
        go(4, tp.y2, tp.yp, rb.at[1, inner], k, hi)
        made[k, 1].wait_recv()
        made[k, 2].wait_recv()
        add_to(part.at[tp.zz, rows], rc.at[0, rows], rc.at[1, rows])
        go(5, tp.zz, tp.zz, rd.at[rows], k, rows)
    begun()
    for k, (rows, lo, hi) in enumerate(cuts):
        inner = pl.ds(k * deep, deep)
        made[k, 3].wait_recv()
        add_to(part.at[tp.ym, lo], rb.at[0, inner])
        go(6, tp.ym, tp.ym, re.at[0, rows], k, rows)
        made[k, 4].wait_recv()
        add_to(part.at[tp.yp, hi], rb.at[1, inner])
        go(7, tp.yp, tp.yp, re.at[1, rows], k, rows)
    for k in range(len(cuts)):
        for at in (5, 6, 7):
            made[k, at].wait_recv()
    total = part[tp.me].astype(F32) + rd[...].astype(F32)
    total = total + re[0].astype(F32) + re[1].astype(F32)
    for one in made.values():
        one.wait_send()
    return total


class SeqGather:
    def __init__(self, seq, buf, first, rows, copy, copy_in):
        self.seq, self.buf, self.copy, self.copy_in = seq, buf, copy, copy_in
        self.all = pl.ds(first, rows)
        self.lo, self.hi = pl.ds(first, rows // 2), pl.ds(first + rows // 2, rows // 2)
        self.sent, self.inner, self.by = [], [], {}

    def go(self, at, slot, rows, to):
        ref = self.buf.at[slot, rows]
        self.by[at] = self.copy(at, ref, ref, to)
        self.sent.append(self.by[at])

    def share(self, slot, rows):
        ref = self.buf.at[slot, rows]
        self.inner.append(self.copy_in(len(self.inner), ref, ref, self.seq.co))

    def start_x(self):
        q = self.seq
        self.go(0, q.me, self.all, q.xp)
        self.go(1, q.me, self.all, q.xm)
        self.share(q.me, self.all)

    def start_h(self):
        self.go(2, self.seq.me, self.all, self.seq.hh)

    def own_row(self):
        q = self.seq
        self.by[0].wait_recv()
        self.go(3, q.xm, self.lo, q.xp)
        self.share(q.xm, self.all)
        self.by[1].wait_recv()
        self.go(4, q.xp, self.hi, q.xm)
        self.share(q.xp, self.all)

    def other_row(self):
        q = self.seq
        self.by[2].wait_recv()
        self.go(5, q.hh, self.all, q.xp)
        self.go(6, q.hh, self.all, q.xm)
        self.share(q.hh, self.all)

    def across(self):
        q = self.seq
        self.by[3].wait_recv()
        self.go(7, q.x2, self.lo, q.hh)
        self.share(q.x2, self.lo)
        self.by[4].wait_recv()
        self.go(8, q.x2, self.hi, q.hh)
        self.share(q.x2, self.hi)

    def far(self):
        q = self.seq
        self.by[5].wait_recv()
        self.share(q.hxm, self.all)
        self.by[6].wait_recv()
        self.share(q.hxp, self.all)

    def end(self):
        q = self.seq
        self.by[7].wait_recv()
        self.share(q.hx2, self.lo)
        self.by[8].wait_recv()
        self.share(q.hx2, self.hi)

    def ready(self):
        for one in self.inner:
            one.wait_recv()

    def sends_done(self):
        for one in self.sent + self.inner:
            one.wait_send()


def norm_factor(buf):
    blocks, rows, wide = buf.shape

    def add(t, squares):
        block = buf[t].astype(F32)
        return squares + jnp.sum(block * block, axis=-1, keepdims=True)

    squares = lax.fori_loop(0, blocks, add, jnp.zeros((rows, 1), F32))
    return lax.rsqrt(squares / (blocks * wide) + EPS)


def turned(block, cosine, sine):
    return block * cosine + pltpu.roll(block, HD // 2, 1) * sine


def layer_kernel(
    lengths,
    freq,
    states_hbm,
    gain_hbm,
    mlp_gain_hbm,
    wq_hbm,
    wk_hbm,
    wv_hbm,
    wo_hbm,
    gate_hbm,
    up_hbm,
    down_hbm,
    out,
    gain,
    mlp_gain,
    begins,
    cosine,
    sine,
    mixed,
    hidden,
    rows_all,
    wq,
    wk,
    wv,
    wo,
    qacc,
    kvacc,
    kv,
    query,
    scores,
    best,
    totals,
    attended,
    part,
    ra,
    rb,
    rc,
    rd,
    re,
    mixed_all,
    normed_mlp,
    gates,
    ups,
    down,
    gate,
    up,
    load,
    s1,
    r1,
    s2,
    r2,
    s3,
    r3,
    s4,
    r4,
    s5,
    r5,
    s6,
    r6,
    s7,
    r7,
    s8,
    r8,
):
    tp, seq = Tp(), Seq()
    tok, wide = states_hbm.shape
    heads = wq.shape[1] // HD
    states = rows_all.at[tp.me]
    units = gate_hbm.shape[1]
    moves = (
        (states_hbm, states),
        (gate_hbm, gates.at[seq.me]),
        (up_hbm, ups.at[seq.me]),
        (down_hbm, down.at[seq.me]),
        (wq_hbm, wq),
        (wk_hbm, wk),
        (wv_hbm, wv),
        (wo_hbm, wo),
        (gain_hbm, gain),
        (mlp_gain_hbm, mlp_gain),
    )
    loads = [pltpu.make_async_copy(a, b, load.at[i]) for i, (a, b) in enumerate(moves)]
    for one in loads[:3]:
        one.start()
    pieces = (gates, ups, down)
    weights = [
        SeqGather(
            seq,
            piece,
            0,
            piece.shape[1],
            sender("seq", s6.at[i], r6.at[i]),
            sender("seq", s7.at[i], r7.at[i]),
        )
        for i, piece in enumerate(pieces)
    ]
    greet(tp, seq)
    loads[0].wait()

    def begun():
        loads[1].wait()
        loads[2].wait()
        weights[0].start_x()
        weights[0].start_h()
        weights[1].start_x()
        weights[1].start_h()
        for one in loads[3:]:
            one.start()
        spots = lax.broadcasted_iota(jnp.int32, (tok, 1), 0) + seq.me * tok
        end, start = 0, jnp.zeros((tok, 1), jnp.int32)
        for k in range(lengths.shape[0]):
            end = end + lengths[k]
            start += jnp.where(spots >= end, lengths[k], 0)
        begins[...] = start
        angle = (spots - start).astype(F32) * freq[...]
        side = jnp.where(lax.broadcasted_iota(jnp.int32, angle.shape, 1) < HD // 2, -1.0, 1.0)
        cosine[...] = jnp.cos(angle)
        sine[...] = jnp.sin(angle) * side

    tp_gather(tp, states, rows_all, sender("tp", s1, r1), begun, idle, idle, False)
    factor = norm_factor(rows_all)
    qacc[...] = jnp.zeros_like(qacc)
    kvacc[...] = jnp.zeros_like(kvacc)
    for one in loads[4:7] + loads[8:]:
        one.wait()

    def project(t, carry):
        normed = (rows_all[t].astype(F32) * factor * gain[t]).astype(BF16)
        at = pl.ds(pl.multiple_of(t * wide, wide), wide)
        qacc[...] += jnp.dot(normed, wq[at, :], preferred_element_type=F32)
        kvacc[:, :HD] += jnp.dot(normed, wk[at, :], preferred_element_type=F32)
        kvacc[:, HD:] += jnp.dot(normed, wv[at, :], preferred_element_type=F32)
        return carry

    lax.fori_loop(0, rows_all.shape[0], project, 0)
    kv[seq.me, :, :HD] = turned(kvacc[:, :HD], cosine[...], sine[...]).astype(BF16)
    kv[seq.me, :, HD:] = kvacc[:, HD:].astype(BF16)
    for h in range(heads):
        block = qacc[:, h * HD : (h + 1) * HD]
        query[h] = turned(block, cosine[...], sine[...]).astype(BF16)
    keys_values = SeqGather(seq, kv, 0, tok, sender("seq", s2, r2), sender("seq", s3, r3))
    keys_values.start_h()
    keys_values.start_x()
    keys_values.own_row()
    keys_values.other_row()
    weights[0].own_row()
    weights[0].other_row()
    keys_values.across()
    loads[3].wait()
    weights[2].start_h()
    weights[1].own_row()
    keys_values.far()
    keys_values.end()
    keys_values.ready()

    blocks = scores.shape[0]
    slots = kv.shape[0]
    best[...] = jnp.full_like(best, -1e30)
    totals[...] = jnp.zeros_like(totals)

    def score(j, carry):
        keys = kv[(seq.me + slots - j) % slots, :, :HD]
        cols = lax.broadcasted_iota(jnp.int32, (tok, tok), 1) + (seq.me - j) * tok
        lines = lax.broadcasted_iota(jnp.int32, (tok, tok), 0) + seq.me * tok
        allowed = (cols >= begins[...]) & (cols <= lines)
        for h in range(heads):
            found = lax.dot_general(
                query[h], keys, (((1,), (1,)), ((), ())), preferred_element_type=F32
            )
            masked = jnp.where(allowed, found * HD ** (-0.5), -1e30)
            scores[j, h] = masked
            best[h] = jnp.maximum(best[h], masked)
        return carry

    lax.fori_loop(0, blocks, score, 0)
    qacc[...] = jnp.zeros_like(qacc)
    highest = [jnp.max(best[h], axis=-1, keepdims=True) for h in range(heads)]
    for h in range(heads):
        best[h] = jnp.broadcast_to(highest[h], (tok, tok))

    def weigh(j, carry):
        values = kv[(seq.me + slots - j) % slots, :, HD:]
        for h in range(heads):
            shares = jnp.exp(scores[j, h] - best[h])
            totals[h] += shares
            qacc[:, h * HD : (h + 1) * HD] += jnp.dot(
                shares.astype(BF16), values, preferred_element_type=F32
            )
        return carry

    lax.fori_loop(0, blocks, weigh, 0)
    for h in range(heads):
        at = slice(h * HD, (h + 1) * HD)
        total = jnp.sum(totals[h], axis=-1, keepdims=True)
        attended[:, at] = (qacc[:, at] / total).astype(BF16)
    loads[7].wait()
    weights[2].start_x()
    weights[1].other_row()

    def fill(slot):
        at = pl.ds(pl.multiple_of(slot * wide, wide), wide)
        part[slot] = jnp.dot(attended[...], wo[:, at], preferred_element_type=F32).astype(BF16)

    def middle():
        weights[0].across()
        weights[0].far()

    def early():
        weights[1].across()
        weights[2].own_row()
        weights[2].other_row()

    def late():
        weights[2].across()
        weights[0].end()
        weights[1].far()

    shares = tp_sum(tp, fill, part, ra, rb, rc, rd, re, sender("tp", s4, r4), middle)
    own = (states[...].astype(F32) + shares).astype(BF16)
    mixed[...] = own
    mixed_all[tp.me] = own
    tp_gather(tp, mixed, mixed_all, sender("tp", s5, r5), early, idle, late, False)
    factor = norm_factor(mixed_all)
    cut = normed_mlp.shape[2]
    for s in range(normed_mlp.shape[0]):
        at = pl.ds(s * cut % wide, cut)
        block = mixed_all[s * cut // wide, :, at].astype(F32)
        normed_mlp[s] = (block * factor * mlp_gain[s]).astype(BF16)
    weights[1].end()
    for one, blocks_of, total in ((weights[0], gates, gate), (weights[1], ups, up)):
        one.ready()
        total[...] = jnp.zeros_like(total)

        def feed(s, carry):
            terms = total[...]
            for k in range(4):
                terms += jnp.dot(
                    normed_mlp[s * 4 + k], blocks_of[s * 4 + k], preferred_element_type=F32
                )
            total[...] = terms
            return carry

        lax.fori_loop(0, normed_mlp.shape[0] // 4, feed, 0)
    hidden[...] = (gate[...] / (1.0 + jnp.exp(-gate[...])) * up[...]).astype(BF16)
    weights[2].far()
    weights[2].end()
    weights[2].ready()

    def fill_down(slot):
        for k in range(wide // cut):
            part[slot, :, k * cut : (k + 1) * cut] = jnp.dot(
                hidden[...], down[slot * (wide // cut) + k], preferred_element_type=F32
            ).astype(BF16)

    shares = tp_sum(tp, fill_down, part, ra, rb, rc, rd, re, sender("tp", s8, r8), idle)
    out[...] = (mixed[...].astype(F32) + shares).astype(BF16)
    for one in [keys_values] + weights:
        one.sends_done()


def sum_scratch(tps, tok, wide):
    return [
        pltpu.VMEM((tps, tok, wide), BF16),
        pltpu.VMEM((tok, wide), BF16),
        pltpu.VMEM((2, tok // 2, wide), BF16),
        pltpu.VMEM((2, tok, wide), BF16),
        pltpu.VMEM((tok, wide), BF16),
        pltpu.VMEM((2, tok, wide), BF16),
    ]


def dma(*counts):
    return [pltpu.SemaphoreType.DMA((n,)) for n in counts]


def per_device(
    states,
    doc_lengths,
    attn_gain,
    query_weight,
    key_weight,
    value_weight,
    output_weight,
    mlp_gain,
    gate_weight,
    up_weight,
    down_weight,
):
    tok, wide = states.shape
    tps, seqs = lax.axis_size("tp"), lax.axis_size("seq")
    heads = query_weight.shape[1] // HD
    depth, units = gate_weight.shape
    half = HD // 2
    freq = THETA ** (-2.0 * np.arange(half) / HD)
    freq = jnp.asarray(np.concatenate([freq, freq])[None, :], F32)
    blocks = min(seqs, 2048 // tok + 1)

    return pl.pallas_call(
        layer_kernel,
        out_shape=jax.ShapeDtypeStruct((tok, wide), BF16),
        in_specs=[pl.BlockSpec(memory_space=pltpu.SMEM), VM] + [ANY] * 10,
        out_specs=VM,
        scratch_shapes=[
            pltpu.VMEM((tps, 1, wide), F32),
            pltpu.VMEM((seqs, 1, depth), F32),
            pltpu.VMEM((tok, 1), jnp.int32),
            pltpu.VMEM((tok, HD), F32),
            pltpu.VMEM((tok, HD), F32),
            pltpu.VMEM((tok, wide), BF16),
            pltpu.VMEM((tok, units), BF16),
            pltpu.VMEM((tps, tok, wide), BF16),
            pltpu.VMEM(query_weight.shape, BF16),
            pltpu.VMEM(key_weight.shape, BF16),
            pltpu.VMEM(value_weight.shape, BF16),
            pltpu.VMEM(output_weight.shape, BF16),
            pltpu.VMEM((tok, heads * HD), F32),
            pltpu.VMEM((tok, 2 * HD), F32),
            pltpu.VMEM((seqs, tok, 2 * HD), BF16),
            pltpu.VMEM((heads, tok, HD), BF16),
            pltpu.VMEM((blocks, heads, tok, tok), F32),
            pltpu.VMEM((heads, tok, tok), F32),
            pltpu.VMEM((heads, tok, tok), F32),
            pltpu.VMEM((tok, heads * HD), BF16),
            *sum_scratch(tps, tok, wide),
            pltpu.VMEM((tps, tok, wide), BF16),
            pltpu.VMEM((seqs, tok, depth), BF16),
            pltpu.VMEM((seqs, depth, units), BF16),
            pltpu.VMEM((seqs, depth, units), BF16),
            pltpu.VMEM((seqs, units, depth), BF16),
            pltpu.VMEM((tok, units), F32),
            pltpu.VMEM((tok, units), F32),
            *dma(10, 36, 36, 9, 9, 10, 10, 32, 32, 36, 36),
            *[pltpu.SemaphoreType.DMA((3, n)) for n in (9, 9, 10, 10)],
            *dma(32, 32),
        ],
        compiler_params=pltpu.CompilerParams(
            collective_id=0, has_side_effects=True, vmem_limit_bytes=67043328
        ),
        cost_estimate=pl.CostEstimate(
            flops=6 * 10**10, bytes_accessed=2 * 10**7, transcendentals=2 * 10**6
        ),
        name="layer",
    )(
        doc_lengths,
        freq,
        states,
        attn_gain.reshape(tps, 1, wide),
        mlp_gain.reshape(seqs, 1, depth),
        query_weight,
        key_weight,
        value_weight,
        output_weight,
        gate_weight,
        up_weight,
        down_weight,
    )


def solution(mesh):
    in_specs = (
        P("seq", "tp"),
        P(),
        P(),
        P(None, "tp"),
        P(None, "tp"),
        P(None, "tp"),
        P("tp", None),
        P(),
        P("seq", "tp"),
        P("seq", "tp"),
        P("tp", "seq"),
    )
    return jax.shard_map(
        per_device, mesh=mesh, in_specs=in_specs, out_specs=P("seq", "tp"), check_vma=False
    )
```
